32 devices in a mesh: radial: 8 (over z, x), phi: 4 (over y, core).
Axes of the slice: x: 2, y: 2, z: 4, core: 2. Of those that a mesh axis runs over, the one named last changes fastest.
Arguments:
- conserved: float32 [8, 64, 64, 128], P(None, 'radial', 'phi'), may hold values from -2.5 to 7, as said below
- core_mass: float32 [1], replicated, may hold values from 0.2 to 1
Outputs:
- advanced: float32 [8, 64, 64, 128], P(None, 'radial', 'phi')
- enclosed_mass: float32 [64], P('radial')
The draws below stay inside these ranges and needn't reach their ends.
Inputs may be any that keep to these rules, and one draw needn't show every extreme that they name: conserved[0] (density) lies between 0.4 and 2.5; conserved[4] exceeds (conserved[1]^2 + conserved[2]^2 + conserved[3]^2)/(2 conserved[0]) by at least 0.6; the speeds |conserved[m]/conserved[0]| stay below 1; conserved[5..7] lie between 0 and conserved[0].
All inputs are finite; a program needn't handle non-finite values.
Results may differ from the reference program's by a relative error of at most 0.0003.
Values sent between devices are 32-bit elements; how exact they have to be, the bound alone decides.
A program may use at most 64 MiB of HBM per device.

```python
import math
import jax
import jax.numpy as jnp
from jax import lax

RD = 8
NT = 128
NR = 64
NP = 64


def draw_conserved(key, part):
    subkeys = jax.random.split(key, 12)
    shape = (NR, NP, NT)
    depth = (jnp.arange(NR, dtype=jnp.float32) + 0.5) / NR
    azimuth = (jnp.arange(NP, dtype=jnp.float32) + 0.5) * (2.0 * math.pi / NP)
    centres = jax.random.uniform(subkeys[6], (3,), jnp.float32, 0.0, 1.0)
    heights = jax.random.uniform(subkeys[7], (3,), jnp.float32, -0.13, 0.13)
    bumps = jnp.exp(-jnp.square((depth[:, None] - centres[None, :]) / 0.15))
    profile = jnp.exp(jnp.sum(bumps * heights[None, :], axis=1))
    turn = jax.random.uniform(subkeys[8], (), jnp.float32, 0.0, 2.0 * math.pi)
    twist = jax.random.uniform(subkeys[9], (), jnp.float32, -0.5 * math.pi, 0.5 * math.pi)
    phase = turn + twist * depth
    angular = 1.0 + 0.35 * jnp.cos(azimuth[None, :] - phase[:, None])
    smooth = (profile[:, None] * angular)[:, :, None]
    rough = jnp.exp(jax.random.uniform(subkeys[0], shape, jnp.float32, jnp.log(0.75), jnp.log(1.33)))
    density = jnp.clip(smooth * rough, 0.4, 2.5)
    speeds = [jnp.clip(0.3 * jax.random.normal(subkeys[1 + which], shape, jnp.float32), -0.99, 0.99) for which in range(3)]
    pressure = jax.random.uniform(subkeys[4], shape, jnp.float32, 0.3, 0.9)
    kinetic = 0.5 * density * (speeds[0] * speeds[0] + speeds[1] * speeds[1] + speeds[2] * speeds[2])
    energy = pressure / (4.0 / 3.0 - 1.0) + kinetic
    tracers = jax.random.uniform(subkeys[5], (3,) + shape, jnp.float32, 0.0, 1.0) * density[None]
    momenta = jnp.stack([density * speeds[0], density * speeds[1], density * speeds[2]])
    return jnp.concatenate([density[None], momenta, energy[None], tracers], axis=0)


def setup_inputs(seed: int = 0) -> dict:
    streams_of = jax.random.split(jax.random.key(seed), 3)
    conserved = draw_conserved(jax.random.fold_in(streams_of[2], 71), 0)
    core_mass = jnp.clip(jnp.exp(jax.random.uniform(streams_of[1], (1,), jnp.float32, math.log(0.2), math.log(1.0))), 0.2, 1.0)
    return {"conserved": conserved, "core_mass": core_mass}


ADIABATIC = 4.0 / 3.0
INNER_RADIUS = 1.0
OUTER_RADIUS = 2.0
COURANT = 0.4
GRAVITY_KICK = 0.004
MINIMUM_DENSITY = 0.05
PRESSURE_FLOOR = 0.01

def step_sizes(radial_total, phi_total, theta_total):
    theta_step = math.pi / theta_total
    phi_step = 2.0 * math.pi / phi_total
    polar_width = INNER_RADIUS * math.sin(0.5 * theta_step) * phi_step
    radial_step = min(2.0 * polar_width, (OUTER_RADIUS - INNER_RADIUS) / radial_total)
    timestep = COURANT * min(radial_step, polar_width)
    return (radial_step, theta_step, phi_step, timestep)

def thermo(values):
    density = jnp.maximum(values[0], MINIMUM_DENSITY)
    kinetic = 0.5 * (values[1] * values[1] + values[2] * values[2] + values[3] * values[3]) / density
    pressure = jnp.maximum((ADIABATIC - 1.0) * (values[4] - kinetic), PRESSURE_FLOOR * density)
    return (density, pressure)

def physical(values, component):
    density, pressure = thermo(values)
    normal = values[component] / density
    sound = jnp.sqrt(ADIABATIC * pressure / density)
    pieces = [values[which] * normal for which in range(values.shape[0])]
    pieces[component] = pieces[component] + pressure
    pieces[4] = pieces[4] + pressure * normal
    return (jnp.stack(pieces), jnp.abs(normal) + sound)

def face_flux(values, along_dim, component):
    interior = values.shape[along_dim] - 4
    neighbour_differences = lax.slice_in_dim(values, 1, interior + 4, axis=along_dim) - lax.slice_in_dim(values, 0, interior + 3, axis=along_dim)
    below_diff = lax.slice_in_dim(neighbour_differences, 0, interior + 2, axis=along_dim)
    above_diff = lax.slice_in_dim(neighbour_differences, 1, interior + 3, axis=along_dim)
    limited = 0.5 * (jnp.sign(below_diff) + jnp.sign(above_diff)) * jnp.minimum(jnp.abs(below_diff), jnp.abs(above_diff))
    left_state = lax.slice_in_dim(values, 1, interior + 2, axis=along_dim) + 0.5 * lax.slice_in_dim(limited, 0, interior + 1, axis=along_dim)
    right_state = lax.slice_in_dim(values, 2, interior + 3, axis=along_dim) - 0.5 * lax.slice_in_dim(limited, 1, interior + 2, axis=along_dim)
    left_flux, left_signal = physical(left_state, component)
    right_flux, right_signal = physical(right_state, component)
    signal = jnp.maximum(left_signal, right_signal)
    return 0.5 * (left_flux + right_flux) - 0.5 * signal * (right_state - left_state)

def hydro_rate(extended, cell_centers, enclosed, radial_step, theta_step, phi_step, strength):
    theta_cells = extended.shape[3]
    centre_cells = extended[:, 2:-2, 2:-2, :]
    polar_padded = jnp.pad(centre_cells, ((0, 0), (0, 0), (0, 0), (2, 2)), mode='edge')
    radial_flux = face_flux(extended[:, :, 2:-2, :], 1, 1)
    polar_flux = face_flux(polar_padded, 3, 2)
    azimuth_flux = face_flux(extended[:, 2:-2, :, :], 2, 3)
    angles = (jnp.arange(theta_cells, dtype=jnp.float32) + 0.5) * theta_step
    sine_center = jnp.sin(angles)
    cosine = jnp.cos(angles)
    face_sine = jnp.sin(jnp.arange(theta_cells + 1, dtype=jnp.float32) * theta_step)
    radius = cell_centers[:, None, None]
    face_radius = jnp.concatenate([cell_centers - 0.5 * radial_step, cell_centers[-1:] + 0.5 * radial_step])[:, None, None]
    radial_area = face_radius * face_radius * radial_flux
    divergence = (radial_area[:, 1:] - radial_area[:, :-1]) / (radius * radius * radial_step)
    polar_area = face_sine * polar_flux
    divergence = divergence + (polar_area[..., 1:] - polar_area[..., :-1]) / (radius * sine_center * theta_step)
    divergence = divergence + (azimuth_flux[:, :, 1:] - azimuth_flux[:, :, :-1]) / (radius * sine_center * phi_step)
    density, pressure = thermo(centre_cells)
    radial_speed = centre_cells[1] / density
    polar_speed = centre_cells[2] / density
    azimuth_speed = centre_cells[3] / density
    cotangent = cosine / sine_center
    gravity_pull = strength * enclosed[:, None, None] / (radius * radius)
    source_radial = (2.0 * pressure + density * (polar_speed * polar_speed + azimuth_speed * azimuth_speed)) / radius - density * gravity_pull
    source_polar = (pressure * cotangent + density * azimuth_speed * azimuth_speed * cotangent - density * radial_speed * polar_speed) / radius
    source_azimuth = -density * azimuth_speed * (radial_speed + polar_speed * cotangent) / radius
    source_energy = -centre_cells[1] * gravity_pull
    nothing = jnp.zeros_like(pressure)
    source = jnp.stack([nothing, source_radial, source_polar, source_azimuth, source_energy, nothing, nothing, nothing])
    return source - divergence

def reference(conserved, core_mass):
    radial_total = conserved.shape[1]
    phi_total = conserved.shape[2]
    theta_total = conserved.shape[3]
    radial_step, theta_step, phi_step, timestep = step_sizes(radial_total, phi_total, theta_total)
    strength = GRAVITY_KICK / timestep
    cell_centers = INNER_RADIUS + (jnp.arange(radial_total, dtype=jnp.float32) + 0.5) * radial_step
    sine_center = jnp.sin((jnp.arange(theta_total, dtype=jnp.float32) + 0.5) * theta_step)
    shells = jnp.dot(lax.optimization_barrier(jnp.sum(conserved[0], axis=1)), sine_center, precision=lax.Precision.HIGHEST)
    shells = shells * cell_centers * cell_centers * (radial_step * theta_step * phi_step)
    enclosed = core_mass[0] + jnp.cumsum(shells) - 0.5 * shells
    blocks = radial_total // RD

    def full_rate(values):
        padded = jnp.pad(values, ((0, 0), (2, 2), (0, 0), (0, 0)), mode='edge')
        padded = jnp.pad(padded, ((0, 0), (0, 0), (2, 2), (0, 0)), mode='wrap')

        def one_block(block_index):
            first_row = (block_index * RD).astype(jnp.int32)
            radial_segment = lax.dynamic_slice_in_dim(padded, first_row, RD + 4, 1)
            radius_part = lax.dynamic_slice_in_dim(cell_centers, first_row, RD, 0)
            mass_part = lax.dynamic_slice_in_dim(enclosed, first_row, RD, 0)
            return hydro_rate(radial_segment, radius_part, mass_part, radial_step, theta_step, phi_step, strength)
        stacked = lax.map(one_block, jnp.arange(blocks, dtype=jnp.int32))
        return jnp.transpose(stacked, (1, 0, 2, 3, 4)).reshape(values.shape)
    section_one = conserved + timestep * full_rate(conserved)
    section_two = section_one + timestep * full_rate(section_one)
    advanced = 0.5 * conserved + 0.5 * section_two
    return (advanced, enclosed)
```

```python
import functools
import math

import jax
import jax.numpy as jnp
import numpy as np
from jax import lax
from jax.experimental import pallas as pl
from jax.experimental.pallas import tpu as pltpu
from jax.sharding import PartitionSpec as P

ADIABATIC = 4.0 / 3.0
INNER_RADIUS = 1.0
OUTER_RADIUS = 2.0
COURANT = 0.4
GRAVITY_KICK = 0.004
MINIMUM_DENSITY = 0.05
PRESSURE_FLOOR = 0.01
MESH = pl.DeviceIdType.MESH
TILE = 8
PAD = 8


def step_sizes(radial_total, phi_total, theta_total):
    theta_step = math.pi / theta_total
    phi_step = 2.0 * math.pi / phi_total
    polar_width = INNER_RADIUS * math.sin(0.5 * theta_step) * phi_step
    radial_step = min(2.0 * polar_width, (OUTER_RADIUS - INNER_RADIUS) / radial_total)
    timestep = COURANT * min(radial_step, polar_width)
    return (radial_step, theta_step, phi_step, timestep)


def angle_tables(theta_cells, theta_step):
    step = np.float32(theta_step)
    centre = (np.arange(theta_cells, dtype=np.float32) + np.float32(0.5)) * step
    face = np.arange(theta_cells + 1, dtype=np.float32) * step
    sine = np.sin(centre.astype(np.float64))
    cosine = np.cos(centre.astype(np.float64))
    face_sine = np.sin(face.astype(np.float64))
    zero = np.zeros(theta_cells)
    rows = [sine, face_sine[:-1], face_sine[1:], cosine / sine, 1.0 / sine, zero, zero, zero]
    return np.stack(rows).astype(np.float32)


def half_slope(below, above):
    return 0.5 * (
        jnp.maximum(jnp.minimum(below, above), 0.0) + jnp.minimum(jnp.maximum(below, above), 0.0)
    )


def thermo(q):
    density = jnp.maximum(q[0], MINIMUM_DENSITY)
    inverse = 1.0 / density
    kinetic = 0.5 * (q[1] * q[1] + q[2] * q[2] + q[3] * q[3]) * inverse
    pressure = jnp.maximum((ADIABATIC - 1.0) * (q[4] - kinetic), PRESSURE_FLOOR * density)
    return density, inverse, pressure


def physical(q, component):
    _, inverse, pressure = thermo(q)
    normal = q[component] * inverse
    squared = ADIABATIC * pressure * inverse
    return normal, pressure, jnp.abs(normal) + squared * lax.rsqrt(squared)


def flux(left, right, component):
    left_v, left_p, left_a = physical(left, component)
    right_v, right_p, right_a = physical(right, component)
    signal = jnp.maximum(left_a, right_a)
    left_w = 0.5 * (left_v + signal)
    right_w = 0.5 * (right_v - signal)
    out = [a * left_w + b * right_w for a, b in zip(left, right)]
    out[component] = out[component] + 0.5 * (left_p + right_p)
    out[4] = out[4] + 0.5 * (left_p * left_v + right_p * right_v)
    return out


def two_faces(rows, component):
    lower_left, lower_right, upper_left, upper_right = [], [], [], []
    for a, b, c, d, e in zip(*rows):
        ab, bc, cd, de = b - a, c - b, d - c, e - d
        sb, sc, sd = half_slope(ab, bc), half_slope(bc, cd), half_slope(cd, de)
        lower_left.append(b + sb)
        lower_right.append(c - sc)
        upper_left.append(c + sc)
        upper_right.append(d - sd)
    return flux(lower_left, lower_right, component), flux(upper_left, upper_right, component)


def kernel(
    sizes,
    counts,
    core_ref,
    table_ref,
    input_ref,
    out_ref,
    mass_ref,
    first,
    second,
    edge,
    halo,
    part,
    slab_part,
    wedge_got,
    slab_got,
    heavy,
    pull,
    table,
    core,
    load_sem,
    radial_send,
    radial_recv,
    phi_send,
    phi_recv,
    wedge_send,
    wedge_recv,
    slab_send,
    slab_recv,
    radial_ready,
    phi_ready,
):
    radial_step, theta_step, phi_step, timestep = sizes
    slabs, wedges = counts
    variables, rows, cells, lanes = input_ref.shape
    tiles = cells // TILE
    strength = GRAVITY_KICK / timestep
    slab, wedge = lax.axis_index("radial"), lax.axis_index("phi")
    has_up, has_down = slab < slabs - 1, slab > 0

    def load(begin, count, sem):
        return pltpu.make_async_copy(
            input_ref.at[:, pl.ds(begin, count)],
            first.at[:, pl.ds(2 + begin, count), pl.ds(PAD, cells), :],
            load_sem.at[sem],
        )

    load_low, load_high, load_inside = load(0, 2, 0), load(rows - 2, 2, 1), load(2, rows - 4, 2)
    load_table = pltpu.make_async_copy(table_ref, table, load_sem.at[3])
    load_core = pltpu.make_async_copy(core_ref, core, load_sem.at[4])
    for copy in (load_low, load_high, load_inside, load_table, load_core):
        copy.start()
    slab_got[...] = jnp.zeros(slab_got.shape, jnp.float32)

    def radial_peer(jump):
        return (lax.rem(slab + jump + slabs, slabs), wedge)

    def phi_peer(jump):
        return (slab, lax.rem(wedge + jump + wedges, wedges))

    barrier = pltpu.get_barrier_semaphore()

    def signal(sem, peer, condition):
        @pl.when(condition)
        def _():
            pl.semaphore_signal(sem, inc=1, device_id=peer, device_id_type=MESH)

    for j in range(1, slabs):
        signal(barrier, radial_peer(j), slab + j < slabs)
    for j in range(1, wedges):
        signal(barrier, phi_peer(j), wedge + j < wedges)
    pl.when(slab + wedge > 0)(lambda: pl.semaphore_wait(barrier, slab + wedge))
    for j in range(1, wedges):
        signal(phi_ready.at[j], phi_peer(-j), wedge >= j)
    for j in range(1, slabs):
        signal(radial_ready.at[j], radial_peer(-j), slab >= j)

    def remote(src, dst, send, recv, peer):
        return pltpu.make_async_remote_copy(
            src_ref=src, dst_ref=dst, send_sem=send, recv_sem=recv, device_id=peer,
            device_id_type=MESH,
        )

    def radial_copies(buffer, section, tile):
        where = pl.ds(PAD + TILE * tile, TILE)
        slot = (section * tiles + tile) * 2
        up = remote(
            buffer.at[:, pl.ds(rows, 2), where, :], buffer.at[:, pl.ds(0, 2), where, :],
            radial_send.at[slot], radial_recv.at[slot], radial_peer(1),
        )
        down = remote(
            buffer.at[:, pl.ds(2, 2), where, :], buffer.at[:, pl.ds(rows + 2, 2), where, :],
            radial_send.at[slot + 1], radial_recv.at[slot + 1], radial_peer(-1),
        )
        return up, down

    first_radial = [radial_copies(first, 0, t) for t in range(tiles)]
    second_radial = [radial_copies(second, 1, t) for t in range(tiles)]

    def up_start(copies):
        pl.when(has_up)(copies[0].start)

    def down_start(copies):
        pl.when(has_down)(copies[1].start)

    whole, inside, low_edge, high_edge = (0, rows), (2, rows - 4), (0, 2), (rows - 2, 2)

    def phi_copies(section, piece, slot):
        where = pl.ds(*piece)
        return [
            remote(
                edge.at[section * 2 + side, :, where], halo.at[section * 2 + side, :, where],
                phi_send.at[slot + side], phi_recv.at[slot + side], phi_peer(jump),
            )
            for side, jump in ((0, -1), (1, 1))
        ]

    def phi_pack(buffer, section, side, piece):
        begin, count = piece
        start = PAD if side == 0 else PAD + cells - 2
        edge[section * 2 + side, :, pl.ds(begin, count)] = buffer[
            :, pl.ds(2 + begin, count), pl.ds(start, 2), :
        ]

    def phi_unpack(buffer, section, side, piece):
        begin, count = piece
        start = PAD + cells if side == 0 else PAD - 2
        buffer[:, pl.ds(2 + begin, count), pl.ds(start, 2), :] = halo[
            section * 2 + side, :, pl.ds(begin, count)
        ]

    first_phi = phi_copies(0, whole, 0)
    inside_phi = phi_copies(1, inside, 2)
    low_phi, high_phi = phi_copies(1, low_edge, 4), phi_copies(1, high_edge, 6)

    wedge_copies = [
        remote(part, wedge_got.at[j], wedge_send.at[j], wedge_recv.at[j], phi_peer(j))
        for j in range(1, wedges)
    ]
    slab_copies = {
        j: remote(slab_part, slab_got.at[j], slab_send.at[j], slab_recv.at[j], radial_peer(j))
        for j in range(1, slabs)
    }
    slab_back = remote(
        slab_part, slab_got.at[0], slab_send.at[0], slab_recv.at[0], radial_peer(-1)
    )

    load_low.wait()
    down_start(first_radial[0])
    load_high.wait()
    load_inside.wait()
    phi_pack(first, 0, 0, whole)
    phi_pack(first, 0, 1, whole)
    for j in range(1, wedges):
        @pl.when(wedge + j < wedges)
        def _():
            pl.semaphore_wait(phi_ready.at[j], 1)
    for copy in first_phi:
        copy.start()

    @pl.when(has_up)
    def _():
        pl.semaphore_wait(radial_ready.at[1], 1)
        for copies in first_radial:
            copies[0].start()

    for copies in first_radial[1:]:
        down_start(copies)

    load_table.wait()
    load_core.wait()
    shape = (TILE, lanes)
    lane = lax.broadcasted_iota(jnp.int32, (rows, lanes), 1)
    line = lax.broadcasted_iota(jnp.int32, (rows, lanes), 0)
    column = jnp.sum(first[0, pl.ds(2, rows), pl.ds(PAD, cells), :], axis=1)
    column = jnp.sum(column * table[0:1, :], axis=1, keepdims=True)
    centres = INNER_RADIUS + (
        (slab * rows + line).astype(jnp.float32) + 0.5
    ) * radial_step
    column = column * centres * centres * (radial_step * theta_step * phi_step)
    part[...] = jnp.sum(jnp.where(lane == line, column, 0.0), axis=0, keepdims=True)
    wedge_got[0] = part[...]
    for copy in wedge_copies:
        copy.start()

    lane_tile = lax.broadcasted_iota(jnp.int32, shape, 1)
    is_first, is_last = lane_tile == 0, lane_tile == lanes - 1

    def rate(buffer, r, tile, radial=True, around_phi=True, along_theta=True):
        start = PAD + TILE * tile

        def at(row, offset):
            where = pl.ds(start + offset, TILE)
            fields = [buffer.at[k] for k in range(variables)]
            if buffer is second:
                fields[1], fields[4] = heavy.at[0], heavy.at[1]
            return [field[row + 2, where, :] for field in fields]

        def spread(value):
            return jnp.broadcast_to(value, shape)

        index = jnp.full(shape, slab * rows + r, jnp.int32).astype(jnp.float32)
        radius = INNER_RADIUS + (index + 0.5) * radial_step
        inner, outer = radius - 0.5 * radial_step, radius + 0.5 * radial_step
        inverse_r = 1.0 / radius
        centre = at(r, 0)
        total = [0.0] * variables
        if radial:
            lower, upper = two_faces([at(r + o, 0) if o else centre for o in range(-2, 3)], 1)
            scale = inverse_r * inverse_r * (1.0 / radial_step)
            area_in, area_out = inner * inner * scale, outer * outer * scale
            total = [area_in * a - area_out * b for a, b in zip(lower, upper)]
        around = inverse_r * spread(table[4:5, :])
        if around_phi:
            lower, upper = two_faces([at(r, o) if o else centre for o in range(-2, 3)], 3)
            scale = around * (1.0 / phi_step)
            total = [t + (a - b) * scale for t, a, b in zip(total, lower, upper)]
        if not along_theta:
            return centre, total
        left, right = [], []
        for q in centre:
            after = jnp.where(is_last, q, pltpu.roll(q, lanes - 1, 1))
            above = after - q
            below = jnp.where(is_first, 0.0, pltpu.roll(above, 1, 1))
            slope = half_slope(below, above)
            left.append(q + slope)
            right.append(jnp.where(is_last, q, pltpu.roll(q - slope, lanes - 1, 1)))
        upper = flux(left, right, 2)
        scale = around * (1.0 / theta_step)
        low_sine, high_sine = spread(table[1:2, :]), spread(table[2:3, :])
        low_area, high_area = low_sine * scale, high_sine * scale
        total = [
            t + (low_area * pltpu.roll(f, 1, 1) - high_area * f) for t, f in zip(total, upper)
        ]
        density, inverse, pressure = thermo(centre)
        vr, vt, vp = (centre[m] * inverse for m in (1, 2, 3))
        cot = spread(table[3:4, :])
        total[1] = total[1] + (2.0 * pressure + density * (vt * vt + vp * vp)) * inverse_r
        total[2] = total[2] + (
            (pressure + density * vp * vp) * cot - density * vr * vt
        ) * inverse_r
        total[3] = total[3] - density * vp * (vr + vt * cot) * inverse_r
        return centre, total

    def first_pass(r, tile, radial):
        centre, total = rate(first, r, tile, radial=radial, around_phi=False)
        where = pl.ds(PAD + TILE * tile, TILE)
        for k in range(variables):
            second[k, r + 2, where, :] = centre[k] + timestep * total[k]

    def add_one(r, tile, **parts):
        _, total = rate(first, r, tile, along_theta=False, **parts)
        where = pl.ds(PAD + TILE * tile, TILE)
        for k in range(variables):
            second[k, r + 2, where, :] = second[k, r + 2, where, :] + timestep * total[k]

    def gravity(p, tile):
        where = pl.ds(PAD + TILE * tile, TILE)
        kick = timestep * jnp.broadcast_to(pull[pl.ds(p, 1), :], shape)
        density = jnp.maximum(first[0, p, where, :], MINIMUM_DENSITY)
        heavy[0, p, where, :] = second[1, p, where, :] - density * kick
        heavy[1, p, where, :] = second[4, p, where, :] - first[1, p, where, :] * kick

    def section_two(r, tile, radial=True):
        centre, total = rate(second, r, tile, radial=radial)
        force = jnp.broadcast_to(pull[pl.ds(r + 2, 1), :], shape)
        density = jnp.maximum(centre[0], MINIMUM_DENSITY)
        total[1] = total[1] - density * force
        total[4] = total[4] - centre[1] * force
        where = pl.ds(PAD + TILE * tile, TILE)
        into = pl.ds(TILE * tile, TILE)
        for k in range(variables):
            begin = first[k, r + 2, where, :]
            out_ref[k, r, into, :] = 0.5 * begin + 0.5 * (centre[k] + timestep * total[k])

    def radial_two(r, tile):
        _, total = rate(second, r, tile, around_phi=False, along_theta=False)
        into = pl.ds(TILE * tile, TILE)
        for k in range(variables):
            out_ref[k, r, into, :] = out_ref[k, r, into, :] + (0.5 * timestep) * total[k]

    def each_row(low, high, step):
        lax.fori_loop(low, high, lambda r, _: (step(r), 0)[1], 0)

    def each_edge(step):
        lax.fori_loop(
            0, 4, lambda i, _: (step(i + (i // 2) * (rows - 4)), 0)[1], 0
        )

    def all_tiles(step):
        def run(r):
            for t in range(tiles):
                step(r, t)

        return run

    def low_land(copies, buffer, tile, after=None):
        where = pl.ds(PAD + TILE * tile, TILE)

        @pl.when(has_down)
        def _():
            copies[0].wait_recv()
            if after:
                after(0, tile)
                after(1, tile)

        @pl.when(jnp.logical_not(has_down))
        def _():
            value = buffer[:, 2, where, :]
            buffer[:, 0, where, :] = value
            buffer[:, 1, where, :] = value
            if buffer is second:
                value = heavy[:, 2, where, :]
                heavy[:, 0, where, :] = value
                heavy[:, 1, where, :] = value

    def high_land(copies, buffer, tile, after=None):
        where = pl.ds(PAD + TILE * tile, TILE)

        @pl.when(has_up)
        def _():
            copies[1].wait_recv()
            if after:
                after(rows + 2, tile)
                after(rows + 3, tile)

        @pl.when(jnp.logical_not(has_up))
        def _():
            value = buffer[:, rows + 1, where, :]
            buffer[:, rows + 2, where, :] = value
            buffer[:, rows + 3, where, :] = value
            if buffer is second:
                value = heavy[:, rows + 1, where, :]
                heavy[:, rows + 2, where, :] = value
                heavy[:, rows + 3, where, :] = value

    def mass_start(low, high):
        for j in range(low, min(high, slabs)):
            @pl.when(slab + j < slabs)
            def _():
                if j > 1:
                    pl.semaphore_wait(radial_ready.at[j], 1)
                slab_copies[j].start()

    each_row(2, rows - 2, all_tiles(lambda r, t: first_pass(r, t, True)))
    for copy in wedge_copies:
        copy.wait_recv()
    shells = jnp.zeros((1, lanes), jnp.float32)
    for w in range(wedges):
        shells = shells + wedge_got[lax.rem(wedge + wedges - w, wedges)]
    slab_part[...] = shells
    pl.when(has_down)(slab_back.start)
    mass_start(1, 3)
    each_edge(all_tiles(lambda r, t: first_pass(r, t, False)))
    for side, copy in enumerate(first_phi):
        copy.wait_recv()
        phi_unpack(first, 0, side, whole)
    each_row(0, rows, all_tiles(lambda r, t: add_one(r, t, radial=False)))
    for side, copy in enumerate(inside_phi):
        phi_pack(second, 1, side, inside)
        copy.start()
    mass_start(3, 5)

    for t in range(tiles):
        low_land(first_radial[t], first, t)
        each_row(0, 2, lambda r: add_one(r, t, around_phi=False))
        down_start(second_radial[t])
    for t in range(tiles):
        high_land(first_radial[t], first, t)
        each_row(rows - 2, rows, lambda r: add_one(r, t, around_phi=False))
        up_start(second_radial[t])
    for side in range(2):
        phi_pack(second, 1, side, low_edge)
        low_phi[side].start()
        phi_pack(second, 1, side, high_edge)
        high_phi[side].start()
    mass_start(5, slabs)

    pl.when(has_up)(slab_back.wait_recv)
    for j in range(1, slabs):
        pl.when(slab >= j)(slab_copies[j].wait_recv)
    before = jnp.zeros((1, lanes), jnp.float32)
    for j in range(slabs - 1, 0, -1):
        before = before + slab_got[j]
    span = (rows + 4, lanes)
    lane = lax.broadcasted_iota(jnp.int32, span, 1)
    line = lax.broadcasted_iota(jnp.int32, span, 0) - 2

    def below(row):
        return jnp.where(lane < row, 1.0, jnp.where(lane == row, 0.5, 0.0))

    def above(row):
        return jnp.where(lane > row, 1.0, jnp.where(lane == row, 0.5, 0.0))

    enclosed = below(line) * slab_part[...] + below(line - rows) * slab_got[0]
    enclosed = enclosed + (before - above(line + rows) * slab_got[1])
    enclosed = core[0] + jnp.sum(enclosed, axis=1, keepdims=True) + jnp.zeros(span, jnp.float32)
    mass_ref[...] = jnp.sum(jnp.where(lane == line, enclosed, 0.0), axis=0, keepdims=True)[:, :rows]
    centres = INNER_RADIUS + (
        (slab * rows + line).astype(jnp.float32) + 0.5
    ) * radial_step
    pull[...] = strength * enclosed / (centres * centres)

    each_row(2, rows + 2, all_tiles(gravity))

    def phi_land(copies, piece):
        begin, count = piece
        for side in range(2):
            copies[side].wait_recv()
            phi_unpack(second, 1, side, piece)
            each_row(2 + begin, 2 + begin + count, lambda p: gravity(p, -1 if side else tiles))

    phi_land(inside_phi, inside)
    each_row(2, rows - 2, all_tiles(section_two))
    phi_land(low_phi, low_edge)
    phi_land(high_phi, high_edge)
    each_edge(all_tiles(lambda r, t: section_two(r, t, False)))
    for t in range(tiles):
        high_land(second_radial[t], second, t, gravity)
        each_row(rows - 2, rows, lambda r: radial_two(r, t))
    for t in range(tiles):
        low_land(second_radial[t], second, t, gravity)
        each_row(0, 2, lambda r: radial_two(r, t))

    for copy in wedge_copies + first_phi + inside_phi + low_phi + high_phi:
        copy.wait_send()
    for j in range(1, slabs):
        pl.when(slab + j < slabs)(slab_copies[j].wait_send)
    pl.when(has_down)(slab_back.wait_send)
    for up, down in first_radial + second_radial:
        pl.when(has_up)(up.wait_send)
        pl.when(has_down)(down.wait_send)


def store(advanced_ref, mass_ref, advanced_out, mass_out, sem):
    copies = [
        pltpu.make_async_copy(advanced_ref, advanced_out, sem.at[0]),
        pltpu.make_async_copy(mass_ref, mass_out, sem.at[1]),
    ]
    for copy in copies:
        copy.start()
    for copy in copies:
        copy.wait()


def body(conserved, core_mass):
    variables, rows, cells, lanes = conserved.shape
    slabs, wedges = lax.axis_size("radial"), lax.axis_size("phi")
    sizes = step_sizes(rows * slabs, cells * wedges, lanes)
    table = jnp.asarray(angle_tables(lanes, sizes[1]))
    tiles = cells // TILE
    padded = (variables, rows + 4, cells + 2 * PAD, lanes)
    vmem = pl.BlockSpec(memory_space=pltpu.VMEM)
    hbm = pl.BlockSpec(memory_space=pltpu.HBM)
    dma = pltpu.SemaphoreType.DMA
    advanced, mass = pl.pallas_call(
        functools.partial(kernel, sizes, (slabs, wedges)),
        out_shape=(
            pltpu.VMEM(conserved.shape, jnp.float32),
            pltpu.VMEM((1, rows), jnp.float32),
        ),
        in_specs=[pl.BlockSpec(memory_space=pl.ANY)] * 3,
        out_specs=(vmem, vmem),
        scratch_shapes=[
            pltpu.VMEM(padded, jnp.float32),
            pltpu.VMEM(padded, jnp.float32),
            pltpu.VMEM((4, variables, rows, 2, lanes), jnp.float32),
            pltpu.VMEM((4, variables, rows, 2, lanes), jnp.float32),
            pltpu.VMEM((1, lanes), jnp.float32),
            pltpu.VMEM((1, lanes), jnp.float32),
            pltpu.VMEM((wedges, 1, lanes), jnp.float32),
            pltpu.VMEM((slabs, 1, lanes), jnp.float32),
            pltpu.VMEM((2,) + padded[1:], jnp.float32),
            pltpu.VMEM((rows + 4, lanes), jnp.float32),
            pltpu.VMEM((TILE, lanes), jnp.float32),
            pltpu.SMEM((1,), jnp.float32),
            dma((5,)),
            dma((4 * tiles,)),
            dma((4 * tiles,)),
            dma((8,)),
            dma((8,)),
            dma((wedges,)),
            dma((wedges,)),
            dma((slabs,)),
            dma((slabs,)),
            pltpu.SemaphoreType.REGULAR((slabs,)),
            pltpu.SemaphoreType.REGULAR((wedges,)),
        ],
        compiler_params=pltpu.CompilerParams(collective_id=0, has_side_effects=True),
    )(core_mass, table, conserved)
    return pl.pallas_call(
        store,
        out_shape=(
            jax.ShapeDtypeStruct(conserved.shape, jnp.float32),
            jax.ShapeDtypeStruct((rows,), jnp.float32),
        ),
        in_specs=[pl.BlockSpec(memory_space=pl.ANY)] * 2,
        out_specs=(hbm, hbm),
        scratch_shapes=[dma((2,))],
        compiler_params=pltpu.CompilerParams(vmem_limit_bytes=4 * 2**20),
    )(advanced, mass.reshape(rows))


def solution(mesh):
    in_specs = (P(None, "radial", "phi", None), P())
    out_specs = (P(None, "radial", "phi", None), P("radial"))
    return jax.shard_map(body, mesh=mesh, in_specs=in_specs, out_specs=out_specs, check_vma=False)
```

```python
import functools
import math

import jax
import jax.numpy as jnp
import numpy as np
from jax import lax
from jax.experimental import pallas as pl
from jax.experimental.pallas import tpu as pltpu
from jax.sharding import PartitionSpec as P

ADIABATIC = 4.0 / 3.0
INNER_RADIUS = 1.0
OUTER_RADIUS = 2.0
COURANT = 0.4
GRAVITY_KICK = 0.004
MINIMUM_DENSITY = 0.05
PRESSURE_FLOOR = 0.01
MESH = pl.DeviceIdType.MESH
TILE = 8
PAD = 8


def step_sizes(radial_total, phi_total, theta_total):
    theta_step = math.pi / theta_total
    phi_step = 2.0 * math.pi / phi_total
    polar_width = INNER_RADIUS * math.sin(0.5 * theta_step) * phi_step
    radial_step = min(2.0 * polar_width, (OUTER_RADIUS - INNER_RADIUS) / radial_total)
    timestep = COURANT * min(radial_step, polar_width)
    return (radial_step, theta_step, phi_step, timestep)


def angle_tables(theta_cells, theta_step):
    step = np.float32(theta_step)
    centre = (np.arange(theta_cells, dtype=np.float32) + np.float32(0.5)) * step
    face = np.arange(theta_cells + 1, dtype=np.float32) * step
    sine = np.sin(centre.astype(np.float64))
    cosine = np.cos(centre.astype(np.float64))
    face_sine = np.sin(face.astype(np.float64))
    zero = np.zeros(theta_cells)
    rows = [sine, face_sine[:-1], face_sine[1:], cosine / sine, 1.0 / sine, zero, zero, zero]
    return np.stack(rows).astype(np.float32)


def half_slope(below, above):
    return 0.5 * (
        jnp.maximum(jnp.minimum(below, above), 0.0) + jnp.minimum(jnp.maximum(below, above), 0.0)
    )


def thermo(q):
    density = jnp.maximum(q[0], MINIMUM_DENSITY)
    inverse = 1.0 / density
    kinetic = 0.5 * (q[1] * q[1] + q[2] * q[2] + q[3] * q[3]) * inverse
    pressure = jnp.maximum((ADIABATIC - 1.0) * (q[4] - kinetic), PRESSURE_FLOOR * density)
    return density, inverse, pressure


def physical(q, component):
    _, inverse, pressure = thermo(q)
    normal = q[component] * inverse
    squared = ADIABATIC * pressure * inverse
    return normal, pressure, jnp.abs(normal) + squared * lax.rsqrt(squared)


def flux(left, right, component):
    left_v, left_p, left_a = physical(left, component)
    right_v, right_p, right_a = physical(right, component)
    signal = jnp.maximum(left_a, right_a)
    left_w = 0.5 * (left_v + signal)
    right_w = 0.5 * (right_v - signal)
    out = [a * left_w + b * right_w for a, b in zip(left, right)]
    out[component] = out[component] + 0.5 * (left_p + right_p)
    out[4] = out[4] + 0.5 * (left_p * left_v + right_p * right_v)
    return out


def two_faces(rows, component):
    lower_left, lower_right, upper_left, upper_right = [], [], [], []
    for a, b, c, d, e in zip(*rows):
        ab, bc, cd, de = b - a, c - b, d - c, e - d
        sb, sc, sd = half_slope(ab, bc), half_slope(bc, cd), half_slope(cd, de)
        lower_left.append(b + sb)
        lower_right.append(c - sc)
        upper_left.append(c + sc)
        upper_right.append(d - sd)
    return flux(lower_left, lower_right, component), flux(upper_left, upper_right, component)


def kernel(
    sizes,
    counts,
    core_ref,
    table_ref,
    input_ref,
    out_ref,
    mass_ref,
    first,
    second,
    edge,
    halo,
    part,
    slab_part,
    wedge_got,
    slab_got,
    heavy,
    pull,
    table,
    core,
    load_sem,
    radial_send,
    radial_recv,
    phi_send,
    phi_recv,
    wedge_send,
    wedge_recv,
    slab_send,
    slab_recv,
    phi_ready,
    slab_ready,
):
    radial_step, theta_step, phi_step, timestep = sizes
    slabs, wedges = counts
    variables, rows, cells, lanes = input_ref.shape
    tiles = cells // TILE
    strength = GRAVITY_KICK / timestep
    slab, wedge = lax.axis_index("radial"), lax.axis_index("phi")
    half = lax.rem(slab, 2)
    is_outer, is_inner = half == 1, half == 0
    has_up, has_down = slab < slabs - 1, slab > 0

    load = pltpu.make_async_copy(
        input_ref, first.at[:, pl.ds(2, rows), pl.ds(PAD, cells), :], load_sem.at[0]
    )
    load_table = pltpu.make_async_copy(table_ref, table, load_sem.at[1])
    load_core = pltpu.make_async_copy(core_ref, core, load_sem.at[2])
    for copy in (load, load_table, load_core):
        copy.start()
    slab_got[...] = jnp.zeros(slab_got.shape, jnp.float32)

    def at_peer(jump, turn=0):
        around = lax.rem(wedge + turn + wedges, wedges) if turn else wedge
        return (lax.rem(slab + jump + slabs, slabs), around)

    barrier = pltpu.get_barrier_semaphore()

    def signal(sem, peer, condition):
        @pl.when(condition)
        def _():
            pl.semaphore_signal(sem, inc=1, device_id=peer, device_id_type=MESH)

    signal(barrier, at_peer(1), has_up)
    signal(barrier, at_peer(-1), has_down)
    for j in range(1, wedges):
        signal(barrier, at_peer(0, j), wedge + j < wedges)
    for j in range(2, slabs):
        signal(barrier, at_peer(j), slab + j < slabs)
    greeted = wedge + slab + jnp.where(has_up, 1, 0)
    def remote(src, dst, send, recv, peer):
        return pltpu.make_async_remote_copy(
            src_ref=src, dst_ref=dst, send_sem=send, recv_sem=recv, device_id=peer,
            device_id_type=MESH,
        )

    def radial_copies(buffer, section, tile):
        where = pl.ds(PAD + TILE * tile, TILE)
        slot = (section * tiles + tile) * 2
        up = remote(
            buffer.at[:, pl.ds(rows, 2), where, :], buffer.at[:, pl.ds(0, 2), where, :],
            radial_send.at[slot], radial_recv.at[slot], at_peer(1),
        )
        down = remote(
            buffer.at[:, pl.ds(2, 2), where, :], buffer.at[:, pl.ds(rows + 2, 2), where, :],
            radial_send.at[slot + 1], radial_recv.at[slot + 1], at_peer(-1),
        )
        return up, down

    first_radial = [radial_copies(first, 0, t) for t in range(tiles)]
    second_radial = [radial_copies(second, 1, t) for t in range(tiles)]

    def up_start(copies):
        pl.when(has_up)(copies[0].start)

    def down_start(copies):
        pl.when(has_down)(copies[1].start)

    whole, inside, low_edge, high_edge = (0, rows), (2, rows - 4), (0, 2), (rows - 2, 2)

    def phi_copies(section, piece, slot):
        where = pl.ds(*piece)
        return [
            remote(
                edge.at[section * 2 + side, :, where], halo.at[section * 2 + side, :, where],
                phi_send.at[slot + side], phi_recv.at[slot + side], at_peer(0, jump),
            )
            for side, jump in ((0, -1), (1, 1))
        ]

    def phi_pack(buffer, section, side, piece):
        begin, count = piece
        start = PAD if side == 0 else PAD + cells - 2
        edge[section * 2 + side, :, pl.ds(begin, count)] = buffer[
            :, pl.ds(2 + begin, count), pl.ds(start, 2), :
        ]

    def phi_unpack(buffer, section, side, piece):
        begin, count = piece
        start = PAD + cells if side == 0 else PAD - 2
        buffer[:, pl.ds(2 + begin, count), pl.ds(start, 2), :] = halo[
            section * 2 + side, :, pl.ds(begin, count)
        ]

    first_phi = phi_copies(0, whole, 0)
    inside_phi = phi_copies(1, inside, 2)
    low_phi, high_phi = phi_copies(1, low_edge, 4), phi_copies(1, high_edge, 6)

    wedge_copies = [
        remote(part, wedge_got.at[j], wedge_send.at[j], wedge_recv.at[j], at_peer(0, j))
        for j in range(1, wedges)
    ]
    slab_copies = {
        j: remote(slab_part, slab_got.at[j], slab_send.at[j], slab_recv.at[j], at_peer(j))
        for j in range(1, slabs)
    }
    slab_back = remote(
        slab_part, slab_got.at[0], slab_send.at[0], slab_recv.at[0], at_peer(-1)
    )
    beside = ((0, wedges - 1), (1, 1))

    load.wait()
    load_table.wait()
    shape = (TILE, lanes)
    lane = lax.broadcasted_iota(jnp.int32, (rows, lanes), 1)
    line = lax.broadcasted_iota(jnp.int32, (rows, lanes), 0)
    column = jnp.sum(first[0, pl.ds(2, rows), pl.ds(PAD, cells), :], axis=1)
    column = jnp.sum(column * table[0:1, :], axis=1, keepdims=True)
    centres = INNER_RADIUS + (
        (slab * rows + line).astype(jnp.float32) + 0.5
    ) * radial_step
    column = column * centres * centres * (radial_step * theta_step * phi_step)
    part[...] = jnp.sum(jnp.where(lane == line, column, 0.0), axis=0, keepdims=True)
    wedge_got[0] = part[...]
    phi_pack(first, 0, 0, whole)
    phi_pack(first, 0, 1, whole)

    lane_tile = lax.broadcasted_iota(jnp.int32, shape, 1)
    is_first, is_last = lane_tile == 0, lane_tile == lanes - 1

    def rate(buffer, r, tile, radial=True, around_phi=True, along_theta=True):
        start = PAD + TILE * tile

        def at(row, offset):
            where = pl.ds(start + offset, TILE)
            fields = [buffer.at[k] for k in range(variables)]
            if buffer is second:
                fields[1], fields[4] = heavy.at[0], heavy.at[1]
            return [field[row + 2, where, :] for field in fields]

        def spread(value):
            return jnp.broadcast_to(value, shape)

        index = jnp.full(shape, slab * rows + r, jnp.int32).astype(jnp.float32)
        radius = INNER_RADIUS + (index + 0.5) * radial_step
        inner, outer = radius - 0.5 * radial_step, radius + 0.5 * radial_step
        inverse_r = 1.0 / radius
        centre = at(r, 0)
        total = [0.0] * variables
        if radial:
            lower, upper = two_faces([at(r + o, 0) if o else centre for o in range(-2, 3)], 1)
            scale = inverse_r * inverse_r * (1.0 / radial_step)
            area_in, area_out = inner * inner * scale, outer * outer * scale
            total = [area_in * a - area_out * b for a, b in zip(lower, upper)]
        around = inverse_r * spread(table[4:5, :])
        if around_phi:
            lower, upper = two_faces([at(r, o) if o else centre for o in range(-2, 3)], 3)
            scale = around * (1.0 / phi_step)
            total = [t + (a - b) * scale for t, a, b in zip(total, lower, upper)]
        if not along_theta:
            return centre, total
        left, right = [], []
        for q in centre:
            after = jnp.where(is_last, q, pltpu.roll(q, lanes - 1, 1))
            above = after - q
            below = jnp.where(is_first, 0.0, pltpu.roll(above, 1, 1))
            slope = half_slope(below, above)
            left.append(q + slope)
            right.append(jnp.where(is_last, q, pltpu.roll(q - slope, lanes - 1, 1)))
        upper = flux(left, right, 2)
        scale = around * (1.0 / theta_step)
        low_sine, high_sine = spread(table[1:2, :]), spread(table[2:3, :])
        low_area, high_area = low_sine * scale, high_sine * scale
        total = [
            t + (low_area * pltpu.roll(f, 1, 1) - high_area * f) for t, f in zip(total, upper)
        ]
        density, inverse, pressure = thermo(centre)
        vr, vt, vp = (centre[m] * inverse for m in (1, 2, 3))
        cot = spread(table[3:4, :])
        total[1] = total[1] + (2.0 * pressure + density * (vt * vt + vp * vp)) * inverse_r
        total[2] = total[2] + (
            (pressure + density * vp * vp) * cot - density * vr * vt
        ) * inverse_r
        total[3] = total[3] - density * vp * (vr + vt * cot) * inverse_r
        return centre, total

    def first_pass(r, tile, radial):
        centre, total = rate(first, r, tile, radial=radial, around_phi=False)
        where = pl.ds(PAD + TILE * tile, TILE)
        for k in range(variables):
            second[k, r + 2, where, :] = centre[k] + timestep * total[k]

    def add_one(r, tile, **parts):
        _, total = rate(first, r, tile, along_theta=False, **parts)
        where = pl.ds(PAD + TILE * tile, TILE)
        for k in range(variables):
            second[k, r + 2, where, :] = second[k, r + 2, where, :] + timestep * total[k]

    def gravity(p, tile):
        where = pl.ds(PAD + TILE * tile, TILE)
        kick = timestep * jnp.broadcast_to(pull[pl.ds(p, 1), :], shape)
        density = jnp.maximum(first[0, p, where, :], MINIMUM_DENSITY)
        heavy[0, p, where, :] = second[1, p, where, :] - density * kick
        heavy[1, p, where, :] = second[4, p, where, :] - first[1, p, where, :] * kick

    def section_two(r, tile, radial=True):
        centre, total = rate(second, r, tile, radial=radial)
        force = jnp.broadcast_to(pull[pl.ds(r + 2, 1), :], shape)
        density = jnp.maximum(centre[0], MINIMUM_DENSITY)
        total[1] = total[1] - density * force
        total[4] = total[4] - centre[1] * force
        where = pl.ds(PAD + TILE * tile, TILE)
        into = pl.ds(TILE * tile, TILE)
        for k in range(variables):
            begin = first[k, r + 2, where, :]
            out_ref[k, r, into, :] = 0.5 * begin + 0.5 * (centre[k] + timestep * total[k])

    def radial_two(r, tile):
        _, total = rate(second, r, tile, around_phi=False, along_theta=False)
        into = pl.ds(TILE * tile, TILE)
        for k in range(variables):
            out_ref[k, r, into, :] = out_ref[k, r, into, :] + (0.5 * timestep) * total[k]

    def each_row(low, high, step):
        lax.fori_loop(low, high, lambda r, _: (step(r), 0)[1], 0)

    def each_edge(step):
        lax.fori_loop(
            0, 4, lambda i, _: (step(i + (i // 2) * (rows - 4)), 0)[1], 0
        )

    def all_tiles(step):
        def run(r):
            for t in range(tiles):
                step(r, t)

        return run

    def low_land(copies, buffer, tile, after=None):
        where = pl.ds(PAD + TILE * tile, TILE)

        @pl.when(has_down)
        def _():
            copies[0].wait_recv()
            if after:
                after(0, tile)
                after(1, tile)

        @pl.when(jnp.logical_not(has_down))
        def _():
            value = buffer[:, 2, where, :]
            buffer[:, 0, where, :] = value
            buffer[:, 1, where, :] = value
            if buffer is second:
                value = heavy[:, 2, where, :]
                heavy[:, 0, where, :] = value
                heavy[:, 1, where, :] = value

    def high_land(copies, buffer, tile, after=None):
        where = pl.ds(PAD + TILE * tile, TILE)

        @pl.when(has_up)
        def _():
            copies[1].wait_recv()
            if after:
                after(rows + 2, tile)
                after(rows + 3, tile)

        @pl.when(jnp.logical_not(has_up))
        def _():
            value = buffer[:, rows + 1, where, :]
            buffer[:, rows + 2, where, :] = value
            buffer[:, rows + 3, where, :] = value
            if buffer is second:
                value = heavy[:, rows + 1, where, :]
                heavy[:, rows + 2, where, :] = value
                heavy[:, rows + 3, where, :] = value

    def slab_start(low, high):
        for j in range(low, min(high, slabs)):
            @pl.when(slab + j < slabs)
            def _():
                if j > 1:
                    pl.semaphore_wait(slab_ready.at[j], 1)
                slab_copies[j].start()

    def interior_one(r, t):
        first_pass(r, t, True)

    def edge_one(r, t):
        first_pass(r, t, False)

    split = jnp.where(has_down, 2, rows - 2)
    each_row(0, 1, all_tiles(edge_one))
    each_row(2, split, all_tiles(interior_one))
    pl.when(greeted > 0)(lambda: pl.semaphore_wait(barrier, greeted))
    for j in range(1, wedges):
        signal(phi_ready.at[j], at_peer(0, -j), wedge >= j)
    for j in range(2, slabs):
        signal(slab_ready.at[j], at_peer(-j), slab >= j)

    def first_down():
        for copies in first_radial:
            down_start(copies)

    for j in range(1, wedges):
        pl.when(wedge + j >= wedges)(wedge_copies[j - 1].start)
    pl.when(is_inner)(first_down)
    for copies in first_radial:
        up_start(copies)
    pl.when(is_outer)(first_down)
    for side, jump in beside:
        pl.when(wedge + jump >= wedges)(first_phi[side].start)
    lax.fori_loop(
        0, 3, lambda i, _: (all_tiles(edge_one)(jnp.where(i == 0, 1, rows - 3 + i)), 0)[1], 0
    )
    for j in range(1, wedges):
        @pl.when(wedge + j < wedges)
        def _():
            pl.semaphore_wait(phi_ready.at[j], 1)
            wedge_copies[j - 1].start()
    for side, jump in beside:
        pl.when(wedge + jump < wedges)(first_phi[side].start)
    each_row(split, rows - 2, all_tiles(interior_one))
    for copy in wedge_copies:
        copy.wait_recv()
    own = jnp.zeros((1, lanes), jnp.float32)
    for w in range(wedges):
        own = own + wedge_got[lax.rem(wedge + wedges - w, wedges)]
    slab_part[...] = own
    pl.when(has_down)(slab_back.start)
    slab_start(1, 4)
    for side, copy in enumerate(first_phi):
        copy.wait_recv()
        phi_unpack(first, 0, side, whole)
    each_edge(all_tiles(lambda r, t: add_one(r, t, radial=False)))

    def radial_side(step, copies, buffer, after, turn, send):
        low = half == step
        base = jnp.where(low, 0, rows - 2)
        for t in range(tiles):
            pl.when(low)(lambda: low_land(copies[t], buffer, t, after))
            pl.when(jnp.logical_not(low))(lambda: high_land(copies[t], buffer, t, after))
            each_row(0, 2, lambda i: turn(base + i, t))
            if send:
                pl.when(low)(lambda: down_start(send[t]))
                pl.when(jnp.logical_not(low))(lambda: up_start(send[t]))

    def radial_one(r, t):
        add_one(r, t, around_phi=False)

    radial_side(0, first_radial, first, None, radial_one, None)
    slab_start(4, 6)
    each_row(2, rows - 2, all_tiles(lambda r, t: add_one(r, t, radial=False)))
    for side, copy in enumerate(inside_phi):
        phi_pack(second, 1, side, inside)
        copy.start()
    for t in range(tiles):
        @pl.when(is_inner)
        def _():
            pl.when(has_up)(first_radial[t][0].wait_send)
            down_start(second_radial[t])

        @pl.when(is_outer)
        def _():
            pl.when(has_down)(first_radial[t][1].wait_send)
            up_start(second_radial[t])

    slab_start(6, slabs)
    radial_side(1, first_radial, first, None, radial_one, second_radial)
    for side in range(2):
        phi_pack(second, 1, side, low_edge)
        low_phi[side].start()
        phi_pack(second, 1, side, high_edge)
        high_phi[side].start()

    load_core.wait()
    pl.when(has_up)(slab_back.wait_recv)
    for j in range(1, slabs):
        pl.when(slab >= j)(slab_copies[j].wait_recv)
    before = jnp.zeros((1, lanes), jnp.float32)
    for j in range(slabs - 1, 0, -1):
        before = before + slab_got[j]
    span = (rows + 4, lanes)
    lane = lax.broadcasted_iota(jnp.int32, span, 1)
    line = lax.broadcasted_iota(jnp.int32, span, 0) - 2

    def below(row):
        return jnp.where(lane < row, 1.0, jnp.where(lane == row, 0.5, 0.0))

    def above(row):
        return jnp.where(lane > row, 1.0, jnp.where(lane == row, 0.5, 0.0))

    enclosed = below(line) * slab_part[...] + below(line - rows) * slab_got[0]
    enclosed = enclosed + (before - above(line + rows) * slab_got[1])
    enclosed = core[0] + jnp.sum(enclosed, axis=1, keepdims=True) + jnp.zeros(span, jnp.float32)
    mass_ref[...] = jnp.sum(jnp.where(lane == line, enclosed, 0.0), axis=0, keepdims=True)[:, :rows]
    centres = INNER_RADIUS + (
        (slab * rows + line).astype(jnp.float32) + 0.5
    ) * radial_step
    pull[...] = strength * enclosed / (centres * centres)

    each_row(2, rows + 2, all_tiles(gravity))

    def phi_land(copies, piece):
        begin, count = piece
        for side in range(2):
            copies[side].wait_recv()
            phi_unpack(second, 1, side, piece)
            each_row(2 + begin, 2 + begin + count, lambda p: gravity(p, -1 if side else tiles))

    phi_land(inside_phi, inside)
    each_row(2, rows - 2, all_tiles(section_two))
    phi_land(low_phi, low_edge)
    phi_land(high_phi, high_edge)
    each_edge(all_tiles(lambda r, t: section_two(r, t, False)))
    radial_side(0, second_radial, second, gravity, radial_two, None)
    radial_side(1, second_radial, second, gravity, radial_two, None)

    for copy in wedge_copies + first_phi + inside_phi + low_phi + high_phi:
        copy.wait_send()
    for j in range(1, slabs):
        pl.when(slab + j < slabs)(slab_copies[j].wait_send)
    pl.when(has_down)(slab_back.wait_send)
    for up, down in first_radial:
        pl.when(has_up & is_outer)(up.wait_send)
        pl.when(has_down & is_inner)(down.wait_send)
    for up, down in second_radial:
        pl.when(has_up)(up.wait_send)
        pl.when(has_down)(down.wait_send)


def store(advanced_ref, mass_ref, advanced_out, mass_out, sem):
    copies = [
        pltpu.make_async_copy(advanced_ref, advanced_out, sem.at[0]),
        pltpu.make_async_copy(mass_ref, mass_out, sem.at[1]),
    ]
    for copy in copies:
        copy.start()
    for copy in copies:
        copy.wait()


def body(conserved, core_mass):
    variables, rows, cells, lanes = conserved.shape
    slabs, wedges = lax.axis_size("radial"), lax.axis_size("phi")
    sizes = step_sizes(rows * slabs, cells * wedges, lanes)
    table = jnp.asarray(angle_tables(lanes, sizes[1]))
    tiles = cells // TILE
    padded = (variables, rows + 4, cells + 2 * PAD, lanes)
    vmem = pl.BlockSpec(memory_space=pltpu.VMEM)
    hbm = pl.BlockSpec(memory_space=pltpu.HBM)
    dma = pltpu.SemaphoreType.DMA
    advanced, mass = pl.pallas_call(
        functools.partial(kernel, sizes, (slabs, wedges)),
        out_shape=(
            pltpu.VMEM(conserved.shape, jnp.float32),
            pltpu.VMEM((1, rows), jnp.float32),
        ),
        in_specs=[pl.BlockSpec(memory_space=pl.ANY)] * 3,
        out_specs=(vmem, vmem),
        scratch_shapes=[
            pltpu.VMEM(padded, jnp.float32),
            pltpu.VMEM(padded, jnp.float32),
            pltpu.VMEM((4, variables, rows, 2, lanes), jnp.float32),
            pltpu.VMEM((4, variables, rows, 2, lanes), jnp.float32),
            pltpu.VMEM((1, lanes), jnp.float32),
            pltpu.VMEM((1, lanes), jnp.float32),
            pltpu.VMEM((wedges, 1, lanes), jnp.float32),
            pltpu.VMEM((slabs, 1, lanes), jnp.float32),
            pltpu.VMEM((2,) + padded[1:], jnp.float32),
            pltpu.VMEM((rows + 4, lanes), jnp.float32),
            pltpu.VMEM((TILE, lanes), jnp.float32),
            pltpu.SMEM((1,), jnp.float32),
            dma((3,)),
            dma((4 * tiles,)),
            dma((4 * tiles,)),
            dma((8,)),
            dma((8,)),
            dma((wedges,)),
            dma((wedges,)),
            dma((slabs,)),
            dma((slabs,)),
            pltpu.SemaphoreType.REGULAR((wedges,)),
            pltpu.SemaphoreType.REGULAR((slabs,)),
        ],
        compiler_params=pltpu.CompilerParams(collective_id=0, has_side_effects=True),
    )(core_mass, table, conserved)
    return pl.pallas_call(
        store,
        out_shape=(
            jax.ShapeDtypeStruct(conserved.shape, jnp.float32),
            jax.ShapeDtypeStruct((rows,), jnp.float32),
        ),
        in_specs=[pl.BlockSpec(memory_space=pl.ANY)] * 2,
        out_specs=(hbm, hbm),
        scratch_shapes=[dma((2,))],
        compiler_params=pltpu.CompilerParams(vmem_limit_bytes=4 * 2**20),
    )(advanced, mass.reshape(rows))


def solution(mesh):
    in_specs = (P(None, "radial", "phi", None), P())
    out_specs = (P(None, "radial", "phi", None), P("radial"))
    return jax.shard_map(body, mesh=mesh, in_specs=in_specs, out_specs=out_specs, check_vma=False)
```

```python
import functools
import math

import jax
import jax.numpy as jnp
import numpy as np
from jax import lax
from jax.experimental import pallas as pl
from jax.experimental.pallas import tpu as pltpu
from jax.sharding import PartitionSpec as P

ADIABATIC = 4.0 / 3.0
INNER_RADIUS = 1.0
OUTER_RADIUS = 2.0
COURANT = 0.4
GRAVITY_KICK = 0.004
MINIMUM_DENSITY = 0.05
PRESSURE_FLOOR = 0.01
MESH = pl.DeviceIdType.MESH
TILE = 8
PAD = 8


def step_sizes(radial_total, phi_total, theta_total):
    theta_step = math.pi / theta_total
    phi_step = 2.0 * math.pi / phi_total
    polar_width = INNER_RADIUS * math.sin(0.5 * theta_step) * phi_step
    radial_step = min(2.0 * polar_width, (OUTER_RADIUS - INNER_RADIUS) / radial_total)
    timestep = COURANT * min(radial_step, polar_width)
    return (radial_step, theta_step, phi_step, timestep)


def angle_tables(theta_cells, theta_step):
    step = np.float32(theta_step)
    centre = (np.arange(theta_cells, dtype=np.float32) + np.float32(0.5)) * step
    face = np.arange(theta_cells + 1, dtype=np.float32) * step
    sine = np.sin(centre.astype(np.float64))
    cosine = np.cos(centre.astype(np.float64))
    face_sine = np.sin(face.astype(np.float64))
    zero = np.zeros(theta_cells)
    rows = [sine, face_sine[:-1], face_sine[1:], cosine / sine, 1.0 / sine, zero, zero, zero]
    return np.stack(rows).astype(np.float32)


def half_slope(below, above):
    return 0.5 * (
        jnp.maximum(jnp.minimum(below, above), 0.0) + jnp.minimum(jnp.maximum(below, above), 0.0)
    )


def thermo(q):
    density = jnp.maximum(q[0], MINIMUM_DENSITY)
    inverse = 1.0 / density
    kinetic = 0.5 * (q[1] * q[1] + q[2] * q[2] + q[3] * q[3]) * inverse
    pressure = jnp.maximum((ADIABATIC - 1.0) * (q[4] - kinetic), PRESSURE_FLOOR * density)
    return density, inverse, pressure


def physical(q, component):
    _, inverse, pressure = thermo(q)
    normal = q[component] * inverse
    squared = ADIABATIC * pressure * inverse
    return normal, pressure, jnp.abs(normal) + squared * lax.rsqrt(squared)


def flux(left, right, component):
    left_v, left_p, left_a = physical(left, component)
    right_v, right_p, right_a = physical(right, component)
    signal = jnp.maximum(left_a, right_a)
    left_w = 0.5 * (left_v + signal)
    right_w = 0.5 * (right_v - signal)
    out = [a * left_w + b * right_w for a, b in zip(left, right)]
    out[component] = out[component] + 0.5 * (left_p + right_p)
    out[4] = out[4] + 0.5 * (left_p * left_v + right_p * right_v)
    return out


def two_faces(rows, component):
    lower_left, lower_right, upper_left, upper_right = [], [], [], []
    for a, b, c, d, e in zip(*rows):
        ab, bc, cd, de = b - a, c - b, d - c, e - d
        sb, sc, sd = half_slope(ab, bc), half_slope(bc, cd), half_slope(cd, de)
        lower_left.append(b + sb)
        lower_right.append(c - sc)
        upper_left.append(c + sc)
        upper_right.append(d - sd)
    return flux(lower_left, lower_right, component), flux(upper_left, upper_right, component)


def kernel(
    sizes,
    counts,
    core_ref,
    table_ref,
    input_ref,
    out_ref,
    mass_ref,
    first,
    second,
    edge,
    halo,
    part,
    slab_part,
    wedge_got,
    slab_got,
    heavy,
    pull,
    table,
    core,
    load_sem,
    radial_send,
    radial_recv,
    phi_send,
    phi_recv,
    wedge_send,
    wedge_recv,
    slab_send,
    slab_recv,
    phi_ready,
    slab_ready,
):
    radial_step, theta_step, phi_step, timestep = sizes
    slabs, wedges = counts
    variables, rows, cells, lanes = input_ref.shape
    tiles = cells // TILE
    strength = GRAVITY_KICK / timestep
    slab, wedge = lax.axis_index("radial"), lax.axis_index("phi")
    half = lax.rem(slab, 2)
    is_outer, is_inner = half == 1, half == 0
    has_up, has_down = slab < slabs - 1, slab > 0

    load = pltpu.make_async_copy(
        input_ref, first.at[:, pl.ds(2, rows), pl.ds(PAD, cells), :], load_sem.at[0]
    )
    load_table = pltpu.make_async_copy(table_ref, table, load_sem.at[1])
    load_core = pltpu.make_async_copy(core_ref, core, load_sem.at[2])
    for copy in (load, load_table, load_core):
        copy.start()
    slab_got[...] = jnp.zeros(slab_got.shape, jnp.float32)

    def at_peer(jump, turn=0):
        around = lax.rem(wedge + turn + wedges, wedges) if turn else wedge
        return (lax.rem(slab + jump + slabs, slabs), around)

    barrier = pltpu.get_barrier_semaphore()

    def signal(sem, peer, condition):
        @pl.when(condition)
        def _():
            pl.semaphore_signal(sem, inc=1, device_id=peer, device_id_type=MESH)

    signal(barrier, at_peer(1), has_up)
    signal(barrier, at_peer(-1), has_down)
    for j in range(1, wedges):
        signal(barrier, at_peer(0, j), wedge + j < wedges)
    for j in range(2, slabs):
        signal(barrier, at_peer(j), slab + j < slabs)
    greeted = wedge + slab + jnp.where(has_up, 1, 0)
    def remote(src, dst, send, recv, peer):
        return pltpu.make_async_remote_copy(
            src_ref=src, dst_ref=dst, send_sem=send, recv_sem=recv, device_id=peer,
            device_id_type=MESH,
        )

    def radial_copies(buffer, section, tile):
        where = pl.ds(PAD + TILE * tile, TILE)
        slot = (section * tiles + tile) * 2
        up = remote(
            buffer.at[:, pl.ds(rows, 2), where, :], buffer.at[:, pl.ds(0, 2), where, :],
            radial_send.at[slot], radial_recv.at[slot], at_peer(1),
        )
        down = remote(
            buffer.at[:, pl.ds(2, 2), where, :], buffer.at[:, pl.ds(rows + 2, 2), where, :],
            radial_send.at[slot + 1], radial_recv.at[slot + 1], at_peer(-1),
        )
        return up, down

    first_radial = [radial_copies(first, 0, t) for t in range(tiles)]
    second_radial = [radial_copies(second, 1, t) for t in range(tiles)]

    def up_start(copies):
        pl.when(has_up)(copies[0].start)

    def down_start(copies):
        pl.when(has_down)(copies[1].start)

    whole = (0, rows)
    main = (jnp.where(is_inner, 0, 2), rows - 2)
    late = (jnp.where(is_inner, rows - 2, 0), 2)

    def phi_copies(section, piece, slot):
        where = pl.ds(*piece)
        return [
            remote(
                edge.at[section * 2 + side, :, where], halo.at[section * 2 + side, :, where],
                phi_send.at[slot + side], phi_recv.at[slot + side], at_peer(0, jump),
            )
            for side, jump in ((0, -1), (1, 1))
        ]

    def phi_pack(buffer, section, side, piece):
        begin, count = piece
        start = PAD if side == 0 else PAD + cells - 2
        edge[section * 2 + side, :, pl.ds(begin, count)] = buffer[
            :, pl.ds(2 + begin, count), pl.ds(start, 2), :
        ]

    def phi_unpack(buffer, section, side, piece):
        begin, count = piece
        start = PAD + cells if side == 0 else PAD - 2
        buffer[:, pl.ds(2 + begin, count), pl.ds(start, 2), :] = halo[
            section * 2 + side, :, pl.ds(begin, count)
        ]

    first_phi = phi_copies(0, whole, 0)
    main_phi, late_phi = phi_copies(1, main, 2), phi_copies(1, late, 4)

    wedge_copies = [
        remote(part, wedge_got.at[j], wedge_send.at[j], wedge_recv.at[j], at_peer(0, j))
        for j in range(1, wedges)
    ]
    slab_copies = {
        j: remote(slab_part, slab_got.at[j], slab_send.at[j], slab_recv.at[j], at_peer(j))
        for j in range(1, slabs)
    }
    slab_back = remote(
        slab_part, slab_got.at[0], slab_send.at[0], slab_recv.at[0], at_peer(-1)
    )
    beside = ((0, wedges - 1), (1, 1))

    load.wait()
    load_table.wait()
    shape = (TILE, lanes)
    lane = lax.broadcasted_iota(jnp.int32, (rows, lanes), 1)
    line = lax.broadcasted_iota(jnp.int32, (rows, lanes), 0)
    column = jnp.sum(first[0, pl.ds(2, rows), pl.ds(PAD, cells), :], axis=1)
    column = jnp.sum(column * table[0:1, :], axis=1, keepdims=True)
    centres = INNER_RADIUS + (
        (slab * rows + line).astype(jnp.float32) + 0.5
    ) * radial_step
    column = column * centres * centres * (radial_step * theta_step * phi_step)
    part[...] = jnp.sum(jnp.where(lane == line, column, 0.0), axis=0, keepdims=True)
    wedge_got[0] = part[...]
    phi_pack(first, 0, 0, whole)
    phi_pack(first, 0, 1, whole)

    lane_tile = lax.broadcasted_iota(jnp.int32, shape, 1)
    is_first, is_last = lane_tile == 0, lane_tile == lanes - 1

    def rate(buffer, r, tile, radial=True, around_phi=True, along_theta=True):
        start = PAD + TILE * tile

        def at(row, offset):
            where = pl.ds(start + offset, TILE)
            fields = [buffer.at[k] for k in range(variables)]
            if buffer is second:
                fields[1], fields[4] = heavy.at[0], heavy.at[1]
            return [field[row + 2, where, :] for field in fields]

        def spread(value):
            return jnp.broadcast_to(value, shape)

        index = jnp.full(shape, slab * rows + r, jnp.int32).astype(jnp.float32)
        radius = INNER_RADIUS + (index + 0.5) * radial_step
        inner, outer = radius - 0.5 * radial_step, radius + 0.5 * radial_step
        inverse_r = 1.0 / radius
        centre = at(r, 0)
        total = [0.0] * variables
        if radial:
            lower, upper = two_faces([at(r + o, 0) if o else centre for o in range(-2, 3)], 1)
            scale = inverse_r * inverse_r * (1.0 / radial_step)
            area_in, area_out = inner * inner * scale, outer * outer * scale
            total = [area_in * a - area_out * b for a, b in zip(lower, upper)]
        around = inverse_r * spread(table[4:5, :])
        if around_phi:
            lower, upper = two_faces([at(r, o) if o else centre for o in range(-2, 3)], 3)
            scale = around * (1.0 / phi_step)
            total = [t + (a - b) * scale for t, a, b in zip(total, lower, upper)]
        if not along_theta:
            return centre, total
        left, right = [], []
        for q in centre:
            after = jnp.where(is_last, q, pltpu.roll(q, lanes - 1, 1))
            above = after - q
            below = jnp.where(is_first, 0.0, pltpu.roll(above, 1, 1))
            slope = half_slope(below, above)
            left.append(q + slope)
            right.append(jnp.where(is_last, q, pltpu.roll(q - slope, lanes - 1, 1)))
        upper = flux(left, right, 2)
        scale = around * (1.0 / theta_step)
        low_sine, high_sine = spread(table[1:2, :]), spread(table[2:3, :])
        low_area, high_area = low_sine * scale, high_sine * scale
        total = [
            t + (low_area * pltpu.roll(f, 1, 1) - high_area * f) for t, f in zip(total, upper)
        ]
        density, inverse, pressure = thermo(centre)
        vr, vt, vp = (centre[m] * inverse for m in (1, 2, 3))
        cot = spread(table[3:4, :])
        total[1] = total[1] + (2.0 * pressure + density * (vt * vt + vp * vp)) * inverse_r
        total[2] = total[2] + (
            (pressure + density * vp * vp) * cot - density * vr * vt
        ) * inverse_r
        total[3] = total[3] - density * vp * (vr + vt * cot) * inverse_r
        return centre, total

    def first_pass(r, tile, radial):
        centre, total = rate(first, r, tile, radial=radial, around_phi=False)
        where = pl.ds(PAD + TILE * tile, TILE)
        for k in range(variables):
            second[k, r + 2, where, :] = centre[k] + timestep * total[k]

    def add_one(r, tile, **parts):
        _, total = rate(first, r, tile, along_theta=False, **parts)
        where = pl.ds(PAD + TILE * tile, TILE)
        for k in range(variables):
            second[k, r + 2, where, :] = second[k, r + 2, where, :] + timestep * total[k]

    def gravity(p, tile):
        where = pl.ds(PAD + TILE * tile, TILE)
        kick = timestep * jnp.broadcast_to(pull[pl.ds(p, 1), :], shape)
        density = jnp.maximum(first[0, p, where, :], MINIMUM_DENSITY)
        heavy[0, p, where, :] = second[1, p, where, :] - density * kick
        heavy[1, p, where, :] = second[4, p, where, :] - first[1, p, where, :] * kick

    def theta_two(r, tile):
        centre, total = rate(second, r, tile, radial=False, around_phi=False)
        force = jnp.broadcast_to(pull[pl.ds(r + 2, 1), :], shape)
        density = jnp.maximum(centre[0], MINIMUM_DENSITY)
        total[1] = total[1] - density * force
        total[4] = total[4] - centre[1] * force
        where = pl.ds(PAD + TILE * tile, TILE)
        into = pl.ds(TILE * tile, TILE)
        for k in range(variables):
            begin = first[k, r + 2, where, :]
            out_ref[k, r, into, :] = 0.5 * begin + 0.5 * (centre[k] + timestep * total[k])

    def phi_two(r, tile):
        _, total = rate(second, r, tile, radial=False, along_theta=False)
        into = pl.ds(TILE * tile, TILE)
        for k in range(variables):
            out_ref[k, r, into, :] = out_ref[k, r, into, :] + (0.5 * timestep) * total[k]

    def radial_two(r, tile):
        _, total = rate(second, r, tile, around_phi=False, along_theta=False)
        into = pl.ds(TILE * tile, TILE)
        for k in range(variables):
            out_ref[k, r, into, :] = out_ref[k, r, into, :] + (0.5 * timestep) * total[k]

    def each_row(low, high, step):
        lax.fori_loop(low, high, lambda r, _: (step(r), 0)[1], 0)

    def each_edge(step):
        lax.fori_loop(
            0, 4, lambda i, _: (step(i + (i // 2) * (rows - 4)), 0)[1], 0
        )

    def all_tiles(step):
        def run(r):
            for t in range(tiles):
                step(r, t)

        return run

    def low_land(copies, buffer, tile, after=None):
        where = pl.ds(PAD + TILE * tile, TILE)

        @pl.when(has_down)
        def _():
            copies[0].wait_recv()
            if after:
                after(0, tile)
                after(1, tile)

        @pl.when(jnp.logical_not(has_down))
        def _():
            value = buffer[:, 2, where, :]
            buffer[:, 0, where, :] = value
            buffer[:, 1, where, :] = value
            if buffer is second:
                value = heavy[:, 2, where, :]
                heavy[:, 0, where, :] = value
                heavy[:, 1, where, :] = value

    def high_land(copies, buffer, tile, after=None):
        where = pl.ds(PAD + TILE * tile, TILE)

        @pl.when(has_up)
        def _():
            copies[1].wait_recv()
            if after:
                after(rows + 2, tile)
                after(rows + 3, tile)

        @pl.when(jnp.logical_not(has_up))
        def _():
            value = buffer[:, rows + 1, where, :]
            buffer[:, rows + 2, where, :] = value
            buffer[:, rows + 3, where, :] = value
            if buffer is second:
                value = heavy[:, rows + 1, where, :]
                heavy[:, rows + 2, where, :] = value
                heavy[:, rows + 3, where, :] = value

    def slab_start(low, high):
        for j in range(low, min(high, slabs)):
            @pl.when(slab + j < slabs)
            def _():
                if j > 1:
                    pl.semaphore_wait(slab_ready.at[j], 1)
                slab_copies[j].start()

    def interior_one(r, t):
        first_pass(r, t, True)

    def edge_one(r, t):
        first_pass(r, t, False)

    split = jnp.where(slab + wedge > 0, 2, rows - 2)
    each_row(0, 1, all_tiles(edge_one))
    each_row(2, split, all_tiles(interior_one))
    pl.when(greeted > 0)(lambda: pl.semaphore_wait(barrier, greeted))
    for j in range(1, wedges):
        signal(phi_ready.at[j], at_peer(0, -j), wedge >= j)
    for j in range(2, slabs):
        signal(slab_ready.at[j], at_peer(-j), slab >= j)

    def first_down():
        for copies in first_radial:
            down_start(copies)

    for j in range(1, wedges):
        pl.when(wedge + j >= wedges)(wedge_copies[j - 1].start)
    pl.when(is_inner)(first_down)
    for copies in first_radial:
        up_start(copies)
    pl.when(is_outer)(first_down)
    for side, jump in beside:
        pl.when(wedge + jump >= wedges)(first_phi[side].start)
    lax.fori_loop(
        0, 3, lambda i, _: (all_tiles(edge_one)(jnp.where(i == 0, 1, rows - 3 + i)), 0)[1], 0
    )
    for j in range(1, wedges):
        @pl.when(wedge + j < wedges)
        def _():
            pl.semaphore_wait(phi_ready.at[j], 1)
            wedge_copies[j - 1].start()
    for side, jump in beside:
        pl.when(wedge + jump < wedges)(first_phi[side].start)
    each_row(split, rows - 2, all_tiles(interior_one))
    for copy in wedge_copies:
        copy.wait_recv()
    own = jnp.zeros((1, lanes), jnp.float32)
    for w in range(wedges):
        own = own + wedge_got[lax.rem(wedge + wedges - w, wedges)]
    slab_part[...] = own
    pl.when(has_down)(slab_back.start)
    slab_start(1, 4)
    for side, copy in enumerate(first_phi):
        copy.wait_recv()
        phi_unpack(first, 0, side, whole)
    each_edge(all_tiles(lambda r, t: add_one(r, t, radial=False)))

    def radial_side(step, copies, buffer, after, turn, send):
        low = half == step
        base = jnp.where(low, 0, rows - 2)
        for t in range(tiles):
            pl.when(low)(lambda: low_land(copies[t], buffer, t, after))
            pl.when(jnp.logical_not(low))(lambda: high_land(copies[t], buffer, t, after))
            each_row(0, 2, lambda i: turn(base + i, t))
            if send:
                pl.when(low)(lambda: down_start(send[t]))
                pl.when(jnp.logical_not(low))(lambda: up_start(send[t]))

    def radial_one(r, t):
        add_one(r, t, around_phi=False)

    def row_of(i):
        return jnp.where(is_inner, i, rows - 1 - i)

    def each_from(low, high, step):
        each_row(low, high, lambda i: step(row_of(i)))

    def passing_start(copies, gates, which):
        for t in range(tiles):
            @pl.when(which)
            def _():
                pl.when(is_inner & has_up)(gates[t][0].wait_send)
                pl.when(is_outer & has_down)(gates[t][1].wait_send)
                pl.when(is_inner)(lambda: down_start(copies[t]))
                pl.when(is_outer)(lambda: up_start(copies[t]))

    def phi_leave(copies, piece):
        for side, copy in enumerate(copies):
            phi_pack(second, 1, side, piece)
            copy.start()

    def phi_land(copies, piece):
        begin, count = piece
        for side in range(2):
            copies[side].wait_recv()
            phi_unpack(second, 1, side, piece)
            each_row(2 + begin, 2 + begin + count, lambda p: gravity(p, -1 if side else tiles))

    span = (rows + 4, lanes)
    lane = lax.broadcasted_iota(jnp.int32, span, 1)
    line = lax.broadcasted_iota(jnp.int32, span, 0) - 2

    def below(row):
        return jnp.where(lane < row, 1.0, jnp.where(lane == row, 0.5, 0.0))

    def above(row):
        return jnp.where(lane > row, 1.0, jnp.where(lane == row, 0.5, 0.0))

    further = INNER_RADIUS + (
        (slab * rows + line).astype(jnp.float32) + 0.5
    ) * radial_step

    def masses():
        load_core.wait()
        for j in range(1, slabs):
            pl.when(slab >= j)(slab_copies[j].wait_recv)
        before = jnp.zeros((1, lanes), jnp.float32)
        for j in range(slabs - 1, 0, -1):
            before = before + slab_got[j]
        enclosed = below(line) * slab_part[...] + (before - above(line + rows) * slab_got[1])
        enclosed = core[0] + jnp.sum(enclosed, axis=1, keepdims=True) + jnp.zeros(span, jnp.float32)
        mass_ref[...] = jnp.sum(jnp.where(lane == line, enclosed, 0.0), axis=0, keepdims=True)[:, :rows]
        pull[...] = strength * enclosed / (further * further)

        each_from(0, rows - 2, all_tiles(lambda r, t: gravity(r + 2, t)))

    slab_start(4, 6)
    radial_side(0, first_radial, first, None, radial_one, None)
    slab_start(6, slabs)
    each_row(2, rows - 2, all_tiles(lambda r, t: add_one(r, t, radial=False)))
    phi_leave(main_phi, main)
    passing_start(second_radial, first_radial, is_inner)
    ahead = jnp.where(is_inner, rows - 4, 0)
    pl.when(is_inner)(masses)
    each_from(0, ahead, all_tiles(theta_two))
    radial_side(1, first_radial, first, None, radial_one, None)
    passing_start(second_radial, first_radial, is_outer)
    for t in range(tiles):
        pl.when(is_inner)(lambda: up_start(second_radial[t]))
        pl.when(is_outer)(lambda: down_start(second_radial[t]))
    phi_leave(late_phi, late)
    pl.when(is_outer)(masses)
    each_from(rows - 2, rows, all_tiles(lambda r, t: gravity(r + 2, t)))
    each_from(ahead, rows, all_tiles(theta_two))
    each_row(2, rows - 2, all_tiles(radial_two))
    phi_land(main_phi, main)
    each_from(0, rows - 2, all_tiles(phi_two))
    phi_land(late_phi, late)
    each_from(rows - 2, rows, all_tiles(phi_two))

    @pl.when(has_up)
    def _():
        slab_back.wait_recv()
        beyond = jnp.sum(below(line - rows) * slab_got[0], axis=1, keepdims=True)
        pull[...] = pull[...] + strength * beyond / (further * further)

    radial_side(0, second_radial, second, gravity, radial_two, None)
    radial_side(1, second_radial, second, gravity, radial_two, None)

    for copy in wedge_copies + first_phi + main_phi + late_phi:
        copy.wait_send()
    for j in range(1, slabs):
        pl.when(slab + j < slabs)(slab_copies[j].wait_send)
    pl.when(has_down)(slab_back.wait_send)
    for up, down in first_radial:
        pl.when(has_up & is_outer)(up.wait_send)
        pl.when(has_down & is_inner)(down.wait_send)
    for up, down in second_radial:
        pl.when(has_up)(up.wait_send)
        pl.when(has_down)(down.wait_send)


def store(advanced_ref, mass_ref, advanced_out, mass_out, sem):
    copies = [
        pltpu.make_async_copy(advanced_ref, advanced_out, sem.at[0]),
        pltpu.make_async_copy(mass_ref, mass_out, sem.at[1]),
    ]
    for copy in copies:
        copy.start()
    for copy in copies:
        copy.wait()


def body(conserved, core_mass):
    variables, rows, cells, lanes = conserved.shape
    slabs, wedges = lax.axis_size("radial"), lax.axis_size("phi")
    sizes = step_sizes(rows * slabs, cells * wedges, lanes)
    table = jnp.asarray(angle_tables(lanes, sizes[1]))
    tiles = cells // TILE
    padded = (variables, rows + 4, cells + 2 * PAD, lanes)
    vmem = pl.BlockSpec(memory_space=pltpu.VMEM)
    hbm = pl.BlockSpec(memory_space=pltpu.HBM)
    dma = pltpu.SemaphoreType.DMA
    advanced, mass = pl.pallas_call(
        functools.partial(kernel, sizes, (slabs, wedges)),
        out_shape=(
            pltpu.VMEM(conserved.shape, jnp.float32),
            pltpu.VMEM((1, rows), jnp.float32),
        ),
        in_specs=[pl.BlockSpec(memory_space=pl.ANY)] * 3,
        out_specs=(vmem, vmem),
        scratch_shapes=[
            pltpu.VMEM(padded, jnp.float32),
            pltpu.VMEM(padded, jnp.float32),
            pltpu.VMEM((4, variables, rows, 2, lanes), jnp.float32),
            pltpu.VMEM((4, variables, rows, 2, lanes), jnp.float32),
            pltpu.VMEM((1, lanes), jnp.float32),
            pltpu.VMEM((1, lanes), jnp.float32),
            pltpu.VMEM((wedges, 1, lanes), jnp.float32),
            pltpu.VMEM((slabs, 1, lanes), jnp.float32),
            pltpu.VMEM((2,) + padded[1:], jnp.float32),
            pltpu.VMEM((rows + 4, lanes), jnp.float32),
            pltpu.VMEM((TILE, lanes), jnp.float32),
            pltpu.SMEM((1,), jnp.float32),
            dma((3,)),
            dma((4 * tiles,)),
            dma((4 * tiles,)),
            dma((8,)),
            dma((8,)),
            dma((wedges,)),
            dma((wedges,)),
            dma((slabs,)),
            dma((slabs,)),
            pltpu.SemaphoreType.REGULAR((wedges,)),
            pltpu.SemaphoreType.REGULAR((slabs,)),
        ],
        compiler_params=pltpu.CompilerParams(collective_id=0, has_side_effects=True),
    )(core_mass, table, conserved)
    return pl.pallas_call(
        store,
        out_shape=(
            jax.ShapeDtypeStruct(conserved.shape, jnp.float32),
            jax.ShapeDtypeStruct((rows,), jnp.float32),
        ),
        in_specs=[pl.BlockSpec(memory_space=pl.ANY)] * 2,
        out_specs=(hbm, hbm),
        scratch_shapes=[dma((2,))],
        compiler_params=pltpu.CompilerParams(vmem_limit_bytes=4 * 2**20),
    )(advanced, mass.reshape(rows))


def solution(mesh):
    in_specs = (P(None, "radial", "phi", None), P())
    out_specs = (P(None, "radial", "phi", None), P("radial"))
    return jax.shard_map(body, mesh=mesh, in_specs=in_specs, out_specs=out_specs, check_vma=False)
```

```python
import functools
import math

import jax
import jax.numpy as jnp
import numpy as np
from jax import lax
from jax.experimental import pallas as pl
from jax.experimental.pallas import tpu as pltpu
from jax.sharding import PartitionSpec as P

ADIABATIC = 4.0 / 3.0
INNER_RADIUS = 1.0
OUTER_RADIUS = 2.0
COURANT = 0.4
GRAVITY_KICK = 0.004
MINIMUM_DENSITY = 0.05
PRESSURE_FLOOR = 0.01
MESH = pl.DeviceIdType.MESH
TILE = 8
PAD = 8


def step_sizes(radial_total, phi_total, theta_total):
    theta_step = math.pi / theta_total
    phi_step = 2.0 * math.pi / phi_total
    polar_width = INNER_RADIUS * math.sin(0.5 * theta_step) * phi_step
    radial_step = min(2.0 * polar_width, (OUTER_RADIUS - INNER_RADIUS) / radial_total)
    timestep = COURANT * min(radial_step, polar_width)
    return (radial_step, theta_step, phi_step, timestep)


def angle_tables(theta_cells, theta_step):
    step = np.float32(theta_step)
    centre = (np.arange(theta_cells, dtype=np.float32) + np.float32(0.5)) * step
    face = np.arange(theta_cells + 1, dtype=np.float32) * step
    sine = np.sin(centre.astype(np.float64))
    cosine = np.cos(centre.astype(np.float64))
    face_sine = np.sin(face.astype(np.float64))
    zero = np.zeros(theta_cells)
    rows = [sine, face_sine[:-1], face_sine[1:], cosine / sine, 1.0 / sine, zero, zero, zero]
    return np.stack(rows).astype(np.float32)


def half_slope(below, above):
    return 0.5 * (
        jnp.maximum(jnp.minimum(below, above), 0.0) + jnp.minimum(jnp.maximum(below, above), 0.0)
    )


def thermo(q):
    density = jnp.maximum(q[0], MINIMUM_DENSITY)
    inverse = 1.0 / density
    kinetic = 0.5 * (q[1] * q[1] + q[2] * q[2] + q[3] * q[3]) * inverse
    pressure = jnp.maximum((ADIABATIC - 1.0) * (q[4] - kinetic), PRESSURE_FLOOR * density)
    return density, inverse, pressure


def physical(q, component):
    _, inverse, pressure = thermo(q)
    normal = q[component] * inverse
    squared = ADIABATIC * pressure * inverse
    return normal, pressure, jnp.abs(normal) + squared * lax.rsqrt(squared)


def flux(left, right, component):
    left_v, left_p, left_a = physical(left, component)
    right_v, right_p, right_a = physical(right, component)
    signal = jnp.maximum(left_a, right_a)
    left_w = 0.5 * (left_v + signal)
    right_w = 0.5 * (right_v - signal)
    out = [a * left_w + b * right_w for a, b in zip(left, right)]
    out[component] = out[component] + 0.5 * (left_p + right_p)
    out[4] = out[4] + 0.5 * (left_p * left_v + right_p * right_v)
    return out


def two_faces(rows, component):
    lower_left, lower_right, upper_left, upper_right = [], [], [], []
    for a, b, c, d, e in zip(*rows):
        ab, bc, cd, de = b - a, c - b, d - c, e - d
        sb, sc, sd = half_slope(ab, bc), half_slope(bc, cd), half_slope(cd, de)
        lower_left.append(b + sb)
        lower_right.append(c - sc)
        upper_left.append(c + sc)
        upper_right.append(d - sd)
    return flux(lower_left, lower_right, component), flux(upper_left, upper_right, component)


def kernel(
    sizes,
    counts,
    core_ref,
    table_ref,
    input_ref,
    out_ref,
    mass_ref,
    first,
    second,
    edge,
    halo,
    part,
    slab_part,
    wedge_got,
    slab_got,
    heavy,
    pull,
    table,
    core,
    load_sem,
    radial_send,
    radial_recv,
    phi_send,
    phi_recv,
    mass_send,
    mass_recv,
    phi_ready,
    slab_ready,
):
    radial_step, theta_step, phi_step, timestep = sizes
    slabs, wedges = counts
    variables, rows, cells, lanes = input_ref.shape
    tiles = cells // TILE
    strength = GRAVITY_KICK / timestep
    slab, wedge = lax.axis_index("radial"), lax.axis_index("phi")
    half = lax.rem(slab, 2)
    is_outer, is_inner = half == 1, half == 0
    has_up, has_down = slab < slabs - 1, slab > 0

    load = pltpu.make_async_copy(
        input_ref, first.at[:, pl.ds(2, rows), pl.ds(PAD, cells), :], load_sem.at[0]
    )
    load_table = pltpu.make_async_copy(table_ref, table, load_sem.at[1])
    load_core = pltpu.make_async_copy(core_ref, core, load_sem.at[2])
    for copy in (load, load_table, load_core):
        copy.start()
    slab_got[...] = jnp.zeros(slab_got.shape, jnp.float32)

    def at_peer(jump, turn=0):
        around = lax.rem(wedge + turn + wedges, wedges) if turn else wedge
        return (lax.rem(slab + jump + slabs, slabs), around)

    barrier = pltpu.get_barrier_semaphore()

    def signal(sem, peer, condition):
        @pl.when(condition)
        def _():
            pl.semaphore_signal(sem, inc=1, device_id=peer, device_id_type=MESH)

    signal(barrier, at_peer(1), has_up)
    signal(barrier, at_peer(-1), has_down)
    for j in range(1, wedges):
        signal(barrier, at_peer(0, j), wedge + j < wedges)
    for j in range(2, slabs):
        signal(barrier, at_peer(j), slab + j < slabs)
    greeted = wedge + slab + jnp.where(has_up, 1, 0)
    def remote(src, dst, send, recv, peer):
        return pltpu.make_async_remote_copy(
            src_ref=src, dst_ref=dst, send_sem=send, recv_sem=recv, device_id=peer,
            device_id_type=MESH,
        )

    def await_bytes(ref, sem):
        pltpu.make_async_copy(ref, ref, sem).wait()

    def radial_copies(buffer, section, tile):
        where = pl.ds(PAD + TILE * tile, TILE)
        slot = (section * tiles + tile) * 2
        up = remote(
            buffer.at[:, pl.ds(rows, 2), where, :], buffer.at[:, pl.ds(0, 2), where, :],
            radial_send.at[slot if section == 0 else 2 * tiles], radial_recv.at[slot], at_peer(1),
        )
        down = remote(
            buffer.at[:, pl.ds(2, 2), where, :], buffer.at[:, pl.ds(rows + 2, 2), where, :],
            radial_send.at[slot + 1 if section == 0 else 2 * tiles], radial_recv.at[slot + 1],
            at_peer(-1),
        )
        return up, down

    first_radial = [radial_copies(first, 0, t) for t in range(tiles)]
    second_radial = [radial_copies(second, 1, t) for t in range(tiles)]

    def up_start(copies):
        pl.when(has_up)(copies[0].start)

    def down_start(copies):
        pl.when(has_down)(copies[1].start)

    whole = (0, rows)
    main = (jnp.where(is_inner, 0, 2), rows - 2)
    late = (jnp.where(is_inner, rows - 2, 0), 2)

    def phi_copies(section, piece, slot):
        where = pl.ds(*piece)
        return [
            remote(
                edge.at[section * 2 + side, :, where], halo.at[section * 2 + side, :, where],
                phi_send.at[0], phi_recv.at[slot], at_peer(0, jump),
            )
            for side, jump in ((0, -1), (1, 1))
        ]

    def phi_pack(buffer, section, side, piece):
        begin, count = piece
        start = PAD if side == 0 else PAD + cells - 2
        edge[section * 2 + side, :, pl.ds(begin, count)] = buffer[
            :, pl.ds(2 + begin, count), pl.ds(start, 2), :
        ]

    def phi_unpack(buffer, section, side, piece):
        begin, count = piece
        start = PAD + cells if side == 0 else PAD - 2
        buffer[:, pl.ds(2 + begin, count), pl.ds(start, 2), :] = halo[
            section * 2 + side, :, pl.ds(begin, count)
        ]

    first_phi = phi_copies(0, whole, 0)
    main_phi, late_phi = phi_copies(1, main, 1), phi_copies(1, late, 2)

    wedge_copies = [
        remote(part, wedge_got.at[j], mass_send.at[0], mass_recv.at[0], at_peer(0, j))
        for j in range(1, wedges)
    ]
    slab_copies = {
        j: remote(slab_part, slab_got.at[j], mass_send.at[1], mass_recv.at[1], at_peer(j))
        for j in range(1, slabs)
    }
    slab_back = remote(
        slab_part, slab_got.at[0], mass_send.at[1], mass_recv.at[2], at_peer(-1)
    )
    beside = ((0, wedges - 1), (1, 1))

    load.wait()
    load_table.wait()
    shape = (TILE, lanes)
    lane = lax.broadcasted_iota(jnp.int32, (rows, lanes), 1)
    line = lax.broadcasted_iota(jnp.int32, (rows, lanes), 0)
    column = jnp.sum(first[0, pl.ds(2, rows), pl.ds(PAD, cells), :], axis=1)
    column = jnp.sum(column * table[0:1, :], axis=1, keepdims=True)
    centres = INNER_RADIUS + (
        (slab * rows + line).astype(jnp.float32) + 0.5
    ) * radial_step
    column = column * centres * centres * (radial_step * theta_step * phi_step)
    part[...] = jnp.sum(jnp.where(lane == line, column, 0.0), axis=0, keepdims=True)
    wedge_got[0] = part[...]
    phi_pack(first, 0, 0, whole)
    phi_pack(first, 0, 1, whole)

    lane_tile = lax.broadcasted_iota(jnp.int32, shape, 1)
    is_first, is_last = lane_tile == 0, lane_tile == lanes - 1

    def rate(buffer, r, tile, radial=True, around_phi=True, along_theta=True):
        start = PAD + TILE * tile

        def at(row, offset):
            where = pl.ds(start + offset, TILE)
            fields = [buffer.at[k] for k in range(variables)]
            if buffer is second:
                fields[1], fields[4] = heavy.at[0], heavy.at[1]
            return [field[row + 2, where, :] for field in fields]

        def spread(value):
            return jnp.broadcast_to(value, shape)

        index = jnp.full(shape, slab * rows + r, jnp.int32).astype(jnp.float32)
        radius = INNER_RADIUS + (index + 0.5) * radial_step
        inner, outer = radius - 0.5 * radial_step, radius + 0.5 * radial_step
        inverse_r = 1.0 / radius
        centre = at(r, 0)
        total = [0.0] * variables
        if radial:
            lower, upper = two_faces([at(r + o, 0) if o else centre for o in range(-2, 3)], 1)
            scale = inverse_r * inverse_r * (1.0 / radial_step)
            area_in, area_out = inner * inner * scale, outer * outer * scale
            total = [area_in * a - area_out * b for a, b in zip(lower, upper)]
        around = inverse_r * spread(table[4:5, :])
        if around_phi:
            lower, upper = two_faces([at(r, o) if o else centre for o in range(-2, 3)], 3)
            scale = around * (1.0 / phi_step)
            total = [t + (a - b) * scale for t, a, b in zip(total, lower, upper)]
        if not along_theta:
            return centre, total
        left, right = [], []
        for q in centre:
            after = jnp.where(is_last, q, pltpu.roll(q, lanes - 1, 1))
            above = after - q
            below = jnp.where(is_first, 0.0, pltpu.roll(above, 1, 1))
            slope = half_slope(below, above)
            left.append(q + slope)
            right.append(jnp.where(is_last, q, pltpu.roll(q - slope, lanes - 1, 1)))
        upper = flux(left, right, 2)
        scale = around * (1.0 / theta_step)
        low_sine, high_sine = spread(table[1:2, :]), spread(table[2:3, :])
        low_area, high_area = low_sine * scale, high_sine * scale
        total = [
            t + (low_area * pltpu.roll(f, 1, 1) - high_area * f) for t, f in zip(total, upper)
        ]
        density, inverse, pressure = thermo(centre)
        vr, vt, vp = (centre[m] * inverse for m in (1, 2, 3))
        cot = spread(table[3:4, :])
        total[1] = total[1] + (2.0 * pressure + density * (vt * vt + vp * vp)) * inverse_r
        total[2] = total[2] + (
            (pressure + density * vp * vp) * cot - density * vr * vt
        ) * inverse_r
        total[3] = total[3] - density * vp * (vr + vt * cot) * inverse_r
        return centre, total

    def first_pass(r, tile, radial):
        centre, total = rate(first, r, tile, radial=radial, around_phi=False)
        where = pl.ds(PAD + TILE * tile, TILE)
        for k in range(variables):
            second[k, r + 2, where, :] = centre[k] + timestep * total[k]

    def add_one(r, tile, **parts):
        _, total = rate(first, r, tile, along_theta=False, **parts)
        where = pl.ds(PAD + TILE * tile, TILE)
        for k in range(variables):
            second[k, r + 2, where, :] = second[k, r + 2, where, :] + timestep * total[k]

    def gravity(p, tile):
        where = pl.ds(PAD + TILE * tile, TILE)
        kick = timestep * jnp.broadcast_to(pull[pl.ds(p, 1), :], shape)
        density = jnp.maximum(first[0, p, where, :], MINIMUM_DENSITY)
        heavy[0, p, where, :] = second[1, p, where, :] - density * kick
        heavy[1, p, where, :] = second[4, p, where, :] - first[1, p, where, :] * kick

    def theta_two(r, tile):
        centre, total = rate(second, r, tile, radial=False, around_phi=False)
        force = jnp.broadcast_to(pull[pl.ds(r + 2, 1), :], shape)
        density = jnp.maximum(centre[0], MINIMUM_DENSITY)
        total[1] = total[1] - density * force
        total[4] = total[4] - centre[1] * force
        where = pl.ds(PAD + TILE * tile, TILE)
        into = pl.ds(TILE * tile, TILE)
        for k in range(variables):
            begin = first[k, r + 2, where, :]
            out_ref[k, r, into, :] = 0.5 * begin + 0.5 * (centre[k] + timestep * total[k])

    def phi_two(r, tile):
        _, total = rate(second, r, tile, radial=False, along_theta=False)
        into = pl.ds(TILE * tile, TILE)
        for k in range(variables):
            out_ref[k, r, into, :] = out_ref[k, r, into, :] + (0.5 * timestep) * total[k]

    def radial_two(r, tile):
        _, total = rate(second, r, tile, around_phi=False, along_theta=False)
        into = pl.ds(TILE * tile, TILE)
        for k in range(variables):
            out_ref[k, r, into, :] = out_ref[k, r, into, :] + (0.5 * timestep) * total[k]

    def each_row(low, high, step):
        lax.fori_loop(low, high, lambda r, _: (step(r), 0)[1], 0)

    def each_edge(step):
        lax.fori_loop(
            0, 4, lambda i, _: (step(i + (i // 2) * (rows - 4)), 0)[1], 0
        )

    def all_tiles(step):
        def run(r):
            for t in range(tiles):
                step(r, t)

        return run

    def low_land(copies, buffer, tile, after=None):
        where = pl.ds(PAD + TILE * tile, TILE)

        @pl.when(has_down)
        def _():
            copies[0].wait_recv()
            if after:
                after(0, tile)
                after(1, tile)

        @pl.when(jnp.logical_not(has_down))
        def _():
            value = buffer[:, 2, where, :]
            buffer[:, 0, where, :] = value
            buffer[:, 1, where, :] = value
            if buffer is second:
                value = heavy[:, 2, where, :]
                heavy[:, 0, where, :] = value
                heavy[:, 1, where, :] = value

    def high_land(copies, buffer, tile, after=None):
        where = pl.ds(PAD + TILE * tile, TILE)

        @pl.when(has_up)
        def _():
            copies[1].wait_recv()
            if after:
                after(rows + 2, tile)
                after(rows + 3, tile)

        @pl.when(jnp.logical_not(has_up))
        def _():
            value = buffer[:, rows + 1, where, :]
            buffer[:, rows + 2, where, :] = value
            buffer[:, rows + 3, where, :] = value
            if buffer is second:
                value = heavy[:, rows + 1, where, :]
                heavy[:, rows + 2, where, :] = value
                heavy[:, rows + 3, where, :] = value

    def slab_start(low, high):
        for j in range(low, min(high, slabs)):
            @pl.when(slab + j < slabs)
            def _():
                if j > 1 and j % 2 == 0:
                    others = 1 if j + 1 >= slabs else 1 + (slab + j + 1 < slabs).astype(jnp.int32)
                    pl.semaphore_wait(slab_ready.at[j // 2 - 1], others)
                slab_copies[j].start()

    def interior_one(r, t):
        first_pass(r, t, True)

    def edge_one(r, t):
        first_pass(r, t, False)

    split = jnp.where(slab + wedge > 0, 2, rows - 2)
    each_row(0, 1, all_tiles(edge_one))
    each_row(2, split, all_tiles(interior_one))
    pl.when(greeted > 0)(lambda: pl.semaphore_wait(barrier, greeted))
    for j in range(1, wedges):
        signal(phi_ready.at[0], at_peer(0, -j), wedge >= j)
    for j in range(2, slabs):
        signal(slab_ready.at[j // 2 - 1], at_peer(-j), slab >= j)

    def first_down():
        for copies in first_radial:
            down_start(copies)

    for j in range(1, wedges):
        pl.when(wedge + j >= wedges)(wedge_copies[j - 1].start)
    pl.when(is_inner)(first_down)
    for copies in first_radial:
        up_start(copies)
    pl.when(is_outer)(first_down)
    for side, jump in beside:
        pl.when(wedge + jump >= wedges)(first_phi[side].start)
    lax.fori_loop(
        0, 3, lambda i, _: (all_tiles(edge_one)(jnp.where(i == 0, 1, rows - 3 + i)), 0)[1], 0
    )

    @pl.when(wedge + 1 < wedges)
    def _():
        pl.semaphore_wait(phi_ready.at[0], wedges - 1 - wedge)

    for j in range(1, wedges):
        pl.when(wedge + j < wedges)(wedge_copies[j - 1].start)
    for side, jump in beside:
        pl.when(wedge + jump < wedges)(first_phi[side].start)
    each_row(split, rows - 2, all_tiles(interior_one))
    await_bytes(wedge_got.at[pl.ds(1, wedges - 1)], mass_recv.at[0])
    own = jnp.zeros((1, lanes), jnp.float32)
    for w in range(wedges):
        own = own + wedge_got[lax.rem(wedge + wedges - w, wedges)]
    slab_part[...] = own
    pl.when(has_down)(slab_back.start)
    slab_start(1, 4)
    await_bytes(halo.at[pl.ds(0, 2)], phi_recv.at[0])
    for side in range(2):
        phi_unpack(first, 0, side, whole)
    each_edge(all_tiles(lambda r, t: add_one(r, t, radial=False)))

    def radial_side(step, copies, buffer, after, turn, send):
        low = half == step
        base = jnp.where(low, 0, rows - 2)
        for t in range(tiles):
            pl.when(low)(lambda: low_land(copies[t], buffer, t, after))
            pl.when(jnp.logical_not(low))(lambda: high_land(copies[t], buffer, t, after))
            each_row(0, 2, lambda i: turn(base + i, t))
            if send:
                pl.when(low)(lambda: down_start(send[t]))
                pl.when(jnp.logical_not(low))(lambda: up_start(send[t]))

    def radial_one(r, t):
        add_one(r, t, around_phi=False)

    def row_of(i):
        return jnp.where(is_inner, i, rows - 1 - i)

    def each_from(low, high, step):
        each_row(low, high, lambda i: step(row_of(i)))

    def passing_start(copies, gates, which, chosen):
        for t in chosen:
            @pl.when(which)
            def _():
                pl.when(is_inner & has_up)(gates[t][0].wait_send)
                pl.when(is_outer & has_down)(gates[t][1].wait_send)
                pl.when(is_inner)(lambda: down_start(copies[t]))
                pl.when(is_outer)(lambda: up_start(copies[t]))

    def phi_leave(copies, piece):
        for side, copy in enumerate(copies):
            phi_pack(second, 1, side, piece)
            copy.start()

    def phi_land(slot, piece):
        begin, count = piece
        await_bytes(halo.at[pl.ds(2, 2), :, pl.ds(begin, count)], phi_recv.at[slot])
        for side in range(2):
            phi_unpack(second, 1, side, piece)
            each_row(2 + begin, 2 + begin + count, lambda p: gravity(p, -1 if side else tiles))

    span = (rows + 4, lanes)
    lane = lax.broadcasted_iota(jnp.int32, span, 1)
    line = lax.broadcasted_iota(jnp.int32, span, 0) - 2

    def below(row):
        return jnp.where(lane < row, 1.0, jnp.where(lane == row, 0.5, 0.0))

    def above(row):
        return jnp.where(lane > row, 1.0, jnp.where(lane == row, 0.5, 0.0))

    further = INNER_RADIUS + (
        (slab * rows + line).astype(jnp.float32) + 0.5
    ) * radial_step

    def masses():
        load_core.wait()
        for j in range(1, slabs):
            @pl.when(slab == j)
            def _():
                await_bytes(slab_got.at[pl.ds(1, j)], mass_recv.at[1])

        before = jnp.zeros((1, lanes), jnp.float32)
        for j in range(slabs - 1, 0, -1):
            before = before + slab_got[j]
        enclosed = below(line) * slab_part[...] + (before - above(line + rows) * slab_got[1])
        enclosed = core[0] + jnp.sum(enclosed, axis=1, keepdims=True) + jnp.zeros(span, jnp.float32)
        mass_ref[...] = jnp.sum(jnp.where(lane == line, enclosed, 0.0), axis=0, keepdims=True)[:, :rows]
        pull[...] = strength * enclosed / (further * further)

        each_from(0, rows - 2, all_tiles(lambda r, t: gravity(r + 2, t)))

    slab_start(4, 6)
    radial_side(0, first_radial, first, None, radial_one, None)
    slab_start(6, slabs)
    passing_start(second_radial, first_radial, is_inner, range(tiles))
    each_row(2, rows - 2, all_tiles(lambda r, t: add_one(r, t, radial=False)))
    phi_leave(main_phi, main)
    passing_start(second_radial, first_radial, is_outer, range(1))
    ahead = jnp.where(is_inner, rows - 4, 0)
    pl.when(is_inner)(masses)
    each_from(0, ahead, all_tiles(theta_two))
    radial_side(1, first_radial, first, None, radial_one, None)
    passing_start(second_radial, first_radial, is_outer, range(1, tiles))
    for t in range(tiles):
        pl.when(is_inner)(lambda: up_start(second_radial[t]))
        pl.when(is_outer)(lambda: down_start(second_radial[t]))
    phi_leave(late_phi, late)
    pl.when(is_outer)(masses)
    each_from(rows - 2, rows, all_tiles(lambda r, t: gravity(r + 2, t)))
    each_from(ahead, rows, all_tiles(theta_two))
    each_row(2, rows - 2, all_tiles(radial_two))
    phi_land(1, main)
    each_from(0, rows - 2, all_tiles(phi_two))
    phi_land(2, late)
    each_from(rows - 2, rows, all_tiles(phi_two))

    @pl.when(has_up)
    def _():
        slab_back.wait_recv()
        beyond = jnp.sum(below(line - rows) * slab_got[0], axis=1, keepdims=True)
        pull[...] = pull[...] + strength * beyond / (further * further)

    radial_side(0, second_radial, second, gravity, radial_two, None)
    radial_side(1, second_radial, second, gravity, radial_two, None)

    await_bytes(halo, phi_send.at[0])
    await_bytes(wedge_got.at[pl.ds(1, wedges - 1)], mass_send.at[0])
    for j in range(slabs):
        @pl.when(slab == j)
        def _():
            await_bytes(slab_got.at[pl.ds(0, slabs - 1 - j + min(j, 1))], mass_send.at[1])

    for up, down in first_radial:
        pl.when(has_up & is_outer)(up.wait_send)
        pl.when(has_down & is_inner)(down.wait_send)
    def second_sent(sides):
        moved = second.at[:, pl.ds(0, 2 * sides), pl.ds(PAD, cells), :]
        await_bytes(moved, radial_send.at[2 * tiles])

    pl.when(has_up & has_down)(lambda: second_sent(2))
    pl.when(has_up != has_down)(lambda: second_sent(1))


def store(advanced_ref, mass_ref, advanced_out, mass_out, sem):
    copies = [
        pltpu.make_async_copy(advanced_ref, advanced_out, sem.at[0]),
        pltpu.make_async_copy(mass_ref, mass_out, sem.at[1]),
    ]
    for copy in copies:
        copy.start()
    for copy in copies:
        copy.wait()


def body(conserved, core_mass):
    variables, rows, cells, lanes = conserved.shape
    slabs, wedges = lax.axis_size("radial"), lax.axis_size("phi")
    sizes = step_sizes(rows * slabs, cells * wedges, lanes)
    table = jnp.asarray(angle_tables(lanes, sizes[1]))
    tiles = cells // TILE
    padded = (variables, rows + 4, cells + 2 * PAD, lanes)
    vmem = pl.BlockSpec(memory_space=pltpu.VMEM)
    hbm = pl.BlockSpec(memory_space=pltpu.HBM)
    dma = pltpu.SemaphoreType.DMA
    advanced, mass = pl.pallas_call(
        functools.partial(kernel, sizes, (slabs, wedges)),
        out_shape=(
            pltpu.VMEM(conserved.shape, jnp.float32),
            pltpu.VMEM((1, rows), jnp.float32),
        ),
        in_specs=[pl.BlockSpec(memory_space=pl.ANY)] * 3,
        out_specs=(vmem, vmem),
        scratch_shapes=[
            pltpu.VMEM(padded, jnp.float32),
            pltpu.VMEM(padded, jnp.float32),
            pltpu.VMEM((4, variables, rows, 2, lanes), jnp.float32),
            pltpu.VMEM((4, variables, rows, 2, lanes), jnp.float32),
            pltpu.VMEM((1, lanes), jnp.float32),
            pltpu.VMEM((1, lanes), jnp.float32),
            pltpu.VMEM((wedges, 1, lanes), jnp.float32),
            pltpu.VMEM((slabs, 1, lanes), jnp.float32),
            pltpu.VMEM((2,) + padded[1:], jnp.float32),
            pltpu.VMEM((rows + 4, lanes), jnp.float32),
            pltpu.VMEM((TILE, lanes), jnp.float32),
            pltpu.SMEM((1,), jnp.float32),
            dma((3,)),
            dma((2 * tiles + 1,)),
            dma((4 * tiles,)),
            dma((1,)),
            dma((3,)),
            dma((2,)),
            dma((3,)),
            pltpu.SemaphoreType.REGULAR((1,)),
            pltpu.SemaphoreType.REGULAR((max(slabs // 2, 1),)),
        ],
        compiler_params=pltpu.CompilerParams(collective_id=0, has_side_effects=True),
    )(core_mass, table, conserved)
    return pl.pallas_call(
        store,
        out_shape=(
            jax.ShapeDtypeStruct(conserved.shape, jnp.float32),
            jax.ShapeDtypeStruct((rows,), jnp.float32),
        ),
        in_specs=[pl.BlockSpec(memory_space=pl.ANY)] * 2,
        out_specs=(hbm, hbm),
        scratch_shapes=[dma((2,))],
        compiler_params=pltpu.CompilerParams(vmem_limit_bytes=4 * 2**20),
    )(advanced, mass.reshape(rows))


def solution(mesh):
    in_specs = (P(None, "radial", "phi", None), P())
    out_specs = (P(None, "radial", "phi", None), P("radial"))
    return jax.shard_map(body, mesh=mesh, in_specs=in_specs, out_specs=out_specs, check_vma=False)
```

```python
import functools
import math

import jax
import jax.numpy as jnp
import numpy as np
from jax import lax
from jax.experimental import pallas as pl
from jax.experimental.pallas import tpu as pltpu
from jax.sharding import PartitionSpec as P

ADIABATIC = 4.0 / 3.0
INNER_RADIUS = 1.0
OUTER_RADIUS = 2.0
COURANT = 0.4
GRAVITY_KICK = 0.004
MINIMUM_DENSITY = 0.05
PRESSURE_FLOOR = 0.01
MESH = pl.DeviceIdType.MESH
TILE = 8
PAD = 8


def step_sizes(radial_total, phi_total, theta_total):
    theta_step = math.pi / theta_total
    phi_step = 2.0 * math.pi / phi_total
    polar_width = INNER_RADIUS * math.sin(0.5 * theta_step) * phi_step
    radial_step = min(2.0 * polar_width, (OUTER_RADIUS - INNER_RADIUS) / radial_total)
    timestep = COURANT * min(radial_step, polar_width)
    return (radial_step, theta_step, phi_step, timestep)


def angle_tables(theta_cells, theta_step):
    step = np.float32(theta_step)
    centre = (np.arange(theta_cells, dtype=np.float32) + np.float32(0.5)) * step
    face = np.arange(theta_cells + 1, dtype=np.float32) * step
    sine = np.sin(centre.astype(np.float64))
    cosine = np.cos(centre.astype(np.float64))
    face_sine = np.sin(face.astype(np.float64))
    zero = np.zeros(theta_cells)
    rows = [sine, face_sine[:-1], face_sine[1:], cosine / sine, 1.0 / sine, zero, zero, zero]
    return np.stack(rows).astype(np.float32)


def half_slope(below, above):
    return 0.5 * jnp.maximum(
        jnp.minimum(below, above), jnp.minimum(jnp.maximum(below, above), 0.0)
    )


def thermo(q):
    density = jnp.maximum(q[0], MINIMUM_DENSITY)
    inverse = 1.0 / density
    kinetic = 0.5 * (q[1] * q[1] + q[2] * q[2] + q[3] * q[3]) * inverse
    pressure = jnp.maximum((ADIABATIC - 1.0) * (q[4] - kinetic), PRESSURE_FLOOR * density)
    return density, inverse, pressure


def physical(q, component):
    _, inverse, pressure = thermo(q)
    normal = q[component] * inverse
    squared = ADIABATIC * pressure * inverse
    return normal, pressure, jnp.abs(normal) + squared * lax.rsqrt(squared)


def flux(left, right, component):
    left_v, left_p, left_a = physical(left, component)
    right_v, right_p, right_a = physical(right, component)
    signal = jnp.maximum(left_a, right_a)
    left_w = 0.5 * (left_v + signal)
    right_w = 0.5 * (right_v - signal)
    out = [a * left_w + b * right_w for a, b in zip(left, right)]
    out[component] = out[component] + 0.5 * (left_p + right_p)
    out[4] = out[4] + 0.5 * (left_p * left_v + right_p * right_v)
    return out


def two_faces(rows, component):
    lower_left, lower_right, upper_left, upper_right = [], [], [], []
    for a, b, c, d, e in zip(*rows):
        ab, bc, cd, de = b - a, c - b, d - c, e - d
        sb, sc, sd = half_slope(ab, bc), half_slope(bc, cd), half_slope(cd, de)
        lower_left.append(b + sb)
        lower_right.append(c - sc)
        upper_left.append(c + sc)
        upper_right.append(d - sd)
    return flux(lower_left, lower_right, component), flux(upper_left, upper_right, component)


def one_face(rows, component):
    left, right = [], []
    for a, b, c, d in zip(*rows):
        ab, bc, cd = b - a, c - b, d - c
        left.append(b + half_slope(ab, bc))
        right.append(c - half_slope(bc, cd))
    return flux(left, right, component)


def kernel(
    sizes,
    counts,
    core_ref,
    table_ref,
    input_ref,
    out_ref,
    mass_ref,
    first,
    second,
    edge,
    halo,
    part,
    slab_part,
    wedge_got,
    slab_got,
    heavy,
    pull,
    table,
    core,
    load_sem,
    radial_send,
    radial_recv,
    phi_send,
    phi_recv,
    mass_send,
    mass_recv,
    phi_ready,
    slab_ready,
):
    radial_step, theta_step, phi_step, timestep = sizes
    slabs, wedges = counts
    variables, rows, cells, lanes = input_ref.shape
    tiles = cells // TILE
    strength = GRAVITY_KICK / timestep
    slab, wedge = lax.axis_index("radial"), lax.axis_index("phi")
    half = lax.rem(slab, 2)
    is_outer, is_inner = half == 1, half == 0
    has_up, has_down = slab < slabs - 1, slab > 0

    load = pltpu.make_async_copy(
        input_ref, first.at[:, pl.ds(2, rows), pl.ds(PAD, cells), :], load_sem.at[0]
    )
    load_table = pltpu.make_async_copy(table_ref, table, load_sem.at[1])
    load_core = pltpu.make_async_copy(core_ref, core, load_sem.at[2])
    for copy in (load, load_table, load_core):
        copy.start()
    slab_got[...] = jnp.zeros(slab_got.shape, jnp.float32)

    def at_peer(jump, turn=0):
        around = lax.rem(wedge + turn + wedges, wedges) if turn else wedge
        return (lax.rem(slab + jump + slabs, slabs), around)

    barrier = pltpu.get_barrier_semaphore()

    def signal(sem, peer, condition):
        @pl.when(condition)
        def _():
            pl.semaphore_signal(sem, inc=1, device_id=peer, device_id_type=MESH)

    signal(barrier, at_peer(1), has_up)
    signal(barrier, at_peer(-1), has_down)
    for j in range(1, wedges):
        signal(barrier, at_peer(0, j), wedge + j < wedges)
    for j in range(2, slabs):
        signal(barrier, at_peer(j), slab + j < slabs)
    greeted = wedge + slab + jnp.where(has_up, 1, 0)
    def remote(src, dst, send, recv, peer):
        return pltpu.make_async_remote_copy(
            src_ref=src, dst_ref=dst, send_sem=send, recv_sem=recv, device_id=peer,
            device_id_type=MESH,
        )

    def await_bytes(ref, sem):
        pltpu.make_async_copy(ref, ref, sem).wait()

    def radial_copies(buffer, section, tile):
        where = pl.ds(PAD + TILE * tile, TILE)
        slot = (section * tiles + tile) * 2
        up = remote(
            buffer.at[:, pl.ds(rows, 2), where, :], buffer.at[:, pl.ds(0, 2), where, :],
            radial_send.at[slot if section == 0 else 2 * tiles], radial_recv.at[slot], at_peer(1),
        )
        down = remote(
            buffer.at[:, pl.ds(2, 2), where, :], buffer.at[:, pl.ds(rows + 2, 2), where, :],
            radial_send.at[slot + 1 if section == 0 else 2 * tiles], radial_recv.at[slot + 1],
            at_peer(-1),
        )
        return up, down

    first_radial = [radial_copies(first, 0, t) for t in range(tiles)]
    second_radial = [radial_copies(second, 1, t) for t in range(tiles)]

    def up_start(copies):
        pl.when(has_up)(copies[0].start)

    def down_start(copies):
        pl.when(has_down)(copies[1].start)

    whole = (0, rows)
    main = (jnp.where(is_inner, 0, 2), rows - 2)
    late = (jnp.where(is_inner, rows - 2, 0), 2)

    def phi_copies(section, piece, slot):
        where = pl.ds(*piece)
        return [
            remote(
                edge.at[section * 2 + side, :, where], halo.at[section * 2 + side, :, where],
                phi_send.at[0], phi_recv.at[slot], at_peer(0, jump),
            )
            for side, jump in ((0, -1), (1, 1))
        ]

    def phi_pack(buffer, section, side, piece):
        begin, count = piece
        start = PAD if side == 0 else PAD + cells - 2
        edge[section * 2 + side, :, pl.ds(begin, count)] = buffer[
            :, pl.ds(2 + begin, count), pl.ds(start, 2), :
        ]

    def phi_unpack(buffer, section, side, piece):
        begin, count = piece
        start = PAD + cells if side == 0 else PAD - 2
        buffer[:, pl.ds(2 + begin, count), pl.ds(start, 2), :] = halo[
            section * 2 + side, :, pl.ds(begin, count)
        ]

    first_phi = phi_copies(0, whole, 0)
    main_phi, late_phi = phi_copies(1, main, 1), phi_copies(1, late, 2)

    wedge_copies = [
        remote(part, wedge_got.at[j], mass_send.at[0], mass_recv.at[0], at_peer(0, j))
        for j in range(1, wedges)
    ]
    slab_copies = {
        j: remote(slab_part, slab_got.at[j], mass_send.at[1], mass_recv.at[1], at_peer(j))
        for j in range(1, slabs)
    }
    slab_back = remote(
        slab_part, slab_got.at[0], mass_send.at[1], mass_recv.at[2], at_peer(-1)
    )
    beside = ((0, wedges - 1), (1, 1))

    load.wait()
    load_table.wait()
    shape = (TILE, lanes)
    lane = lax.broadcasted_iota(jnp.int32, (rows, lanes), 1)
    line = lax.broadcasted_iota(jnp.int32, (rows, lanes), 0)
    column = jnp.sum(first[0, pl.ds(2, rows), pl.ds(PAD, cells), :], axis=1)
    column = jnp.sum(column * table[0:1, :], axis=1, keepdims=True)
    centres = INNER_RADIUS + (
        (slab * rows + line).astype(jnp.float32) + 0.5
    ) * radial_step
    column = column * centres * centres * (radial_step * theta_step * phi_step)
    part[...] = jnp.sum(jnp.where(lane == line, column, 0.0), axis=0, keepdims=True)
    wedge_got[0] = part[...]
    phi_pack(first, 0, 0, whole)
    phi_pack(first, 0, 1, whole)

    lane_tile = lax.broadcasted_iota(jnp.int32, shape, 1)
    is_first, is_last = lane_tile == 0, lane_tile == lanes - 1

    def fields_at(buffer, row, start):
        where = pl.ds(start, TILE)
        fields = [buffer.at[k] for k in range(variables)]
        if buffer is second:
            fields[1], fields[4] = heavy.at[0], heavy.at[1]
        return [field[row + 2, where, :] for field in fields]

    def radius_at(position):
        step = jnp.full(shape, slab * rows + position, jnp.int32).astype(jnp.float32)
        return INNER_RADIUS + step * radial_step

    def face_scale(face, row):
        area, inverse_r = radius_at(face), 1.0 / (radius_at(row) + 0.5 * radial_step)
        return area * area * (inverse_r * inverse_r * (1.0 / radial_step))

    def add_flux(buffer, row, tile, scale, values):
        if buffer is first:
            target, row, start, step = second, row + 2, PAD + TILE * tile, timestep
        else:
            target, start, step = out_ref, TILE * tile, 0.5 * timestep
        scale = scale * step
        where = pl.ds(start, TILE)
        for k in range(variables):
            target[k, row, where, :] = target[k, row, where, :] + scale * values[k]

    def inner_face(buffer, face, tile):
        start = PAD + TILE * tile
        values = one_face([fields_at(buffer, face + o, start) for o in range(-2, 2)], 1)
        add_flux(buffer, face - 1, tile, -face_scale(face, face - 1), values)
        add_flux(buffer, face, tile, face_scale(face, face), values)

    def side_faces(buffer, low, tile):
        start = PAD + TILE * tile
        edge_row = jnp.where(low, 0, rows - 1)
        next_row = jnp.where(low, 1, rows - 2)
        lower, upper = two_faces([fields_at(buffer, edge_row + o, start) for o in range(-2, 3)], 1)
        low_scale, high_scale = face_scale(edge_row, edge_row), face_scale(edge_row + 1, edge_row)
        values = [low_scale * a - high_scale * b for a, b in zip(lower, upper)]
        add_flux(buffer, edge_row, tile, 1.0, values)
        between = [jnp.where(low, b, a) for a, b in zip(lower, upper)]
        scale = face_scale(jnp.where(low, 1, rows - 1), next_row)
        add_flux(buffer, next_row, tile, jnp.where(low, scale, -scale), between)

    def rate(buffer, r, tile, around_phi=True, along_theta=True):
        start = PAD + TILE * tile

        def at(row, offset):
            return fields_at(buffer, row, start + offset)

        def spread(value):
            return jnp.broadcast_to(value, shape)

        index = jnp.full(shape, slab * rows + r, jnp.int32).astype(jnp.float32)
        radius = INNER_RADIUS + (index + 0.5) * radial_step
        inverse_r = 1.0 / radius
        centre = at(r, 0)
        total = [0.0] * variables
        around = inverse_r * spread(table[4:5, :])
        if around_phi:
            lower, upper = two_faces([at(r, o) if o else centre for o in range(-2, 3)], 3)
            scale = around * (1.0 / phi_step)
            total = [t + (a - b) * scale for t, a, b in zip(total, lower, upper)]
        if not along_theta:
            return centre, total
        left, right = [], []
        for q in centre:
            after = jnp.where(is_last, q, pltpu.roll(q, lanes - 1, 1))
            above = after - q
            below = jnp.where(is_first, 0.0, pltpu.roll(above, 1, 1))
            slope = half_slope(below, above)
            left.append(q + slope)
            right.append(jnp.where(is_last, q, pltpu.roll(q - slope, lanes - 1, 1)))
        upper = flux(left, right, 2)
        scale = around * (1.0 / theta_step)
        low_sine, high_sine = spread(table[1:2, :]), spread(table[2:3, :])
        low_area, high_area = low_sine * scale, high_sine * scale
        total = [
            t + (low_area * pltpu.roll(f, 1, 1) - high_area * f) for t, f in zip(total, upper)
        ]
        density, inverse, pressure = thermo(centre)
        vr, vt, vp = (centre[m] * inverse for m in (1, 2, 3))
        cot = spread(table[3:4, :])
        total[1] = total[1] + (2.0 * pressure + density * (vt * vt + vp * vp)) * inverse_r
        total[2] = total[2] + (
            (pressure + density * vp * vp) * cot - density * vr * vt
        ) * inverse_r
        total[3] = total[3] - density * vp * (vr + vt * cot) * inverse_r
        return centre, total

    def first_pass(r, tile):
        centre, total = rate(first, r, tile, around_phi=False)
        where = pl.ds(PAD + TILE * tile, TILE)
        for k in range(variables):
            second[k, r + 2, where, :] = centre[k] + timestep * total[k]

    def phi_one(r, tile):
        _, total = rate(first, r, tile, along_theta=False)
        where = pl.ds(PAD + TILE * tile, TILE)
        for k in range(variables):
            second[k, r + 2, where, :] = second[k, r + 2, where, :] + timestep * total[k]

    def gravity(p, tile):
        where = pl.ds(PAD + TILE * tile, TILE)
        kick = timestep * jnp.broadcast_to(pull[pl.ds(p, 1), :], shape)
        density = jnp.maximum(first[0, p, where, :], MINIMUM_DENSITY)
        heavy[0, p, where, :] = second[1, p, where, :] - density * kick
        heavy[1, p, where, :] = second[4, p, where, :] - first[1, p, where, :] * kick

    def theta_two(r, tile):
        centre, total = rate(second, r, tile, around_phi=False)
        force = jnp.broadcast_to(pull[pl.ds(r + 2, 1), :], shape)
        density = jnp.maximum(centre[0], MINIMUM_DENSITY)
        total[1] = total[1] - density * force
        total[4] = total[4] - centre[1] * force
        where = pl.ds(PAD + TILE * tile, TILE)
        into = pl.ds(TILE * tile, TILE)
        for k in range(variables):
            begin = first[k, r + 2, where, :]
            out_ref[k, r, into, :] = 0.5 * begin + 0.5 * (centre[k] + timestep * total[k])

    def phi_two(r, tile):
        _, total = rate(second, r, tile, along_theta=False)
        into = pl.ds(TILE * tile, TILE)
        for k in range(variables):
            out_ref[k, r, into, :] = out_ref[k, r, into, :] + (0.5 * timestep) * total[k]

    def each_row(low, high, step):
        lax.fori_loop(low, high, lambda r, _: (step(r), 0)[1], 0)

    def each_edge(step):
        lax.fori_loop(
            0, 4, lambda i, _: (step(i + (i // 2) * (rows - 4)), 0)[1], 0
        )

    def all_tiles(step):
        def run(r):
            for t in range(tiles):
                step(r, t)

        return run

    def low_land(copies, buffer, tile, after=None):
        where = pl.ds(PAD + TILE * tile, TILE)

        @pl.when(has_down)
        def _():
            copies[0].wait_recv()
            if after:
                after(0, tile)
                after(1, tile)

        @pl.when(jnp.logical_not(has_down))
        def _():
            value = buffer[:, 2, where, :]
            buffer[:, 0, where, :] = value
            buffer[:, 1, where, :] = value
            if buffer is second:
                value = heavy[:, 2, where, :]
                heavy[:, 0, where, :] = value
                heavy[:, 1, where, :] = value

    def high_land(copies, buffer, tile, after=None):
        where = pl.ds(PAD + TILE * tile, TILE)

        @pl.when(has_up)
        def _():
            copies[1].wait_recv()
            if after:
                after(rows + 2, tile)
                after(rows + 3, tile)

        @pl.when(jnp.logical_not(has_up))
        def _():
            value = buffer[:, rows + 1, where, :]
            buffer[:, rows + 2, where, :] = value
            buffer[:, rows + 3, where, :] = value
            if buffer is second:
                value = heavy[:, rows + 1, where, :]
                heavy[:, rows + 2, where, :] = value
                heavy[:, rows + 3, where, :] = value

    def slab_start(low, high):
        for j in range(low, min(high, slabs)):
            @pl.when(slab + j < slabs)
            def _():
                if j > 1 and j % 2 == 0:
                    others = 1 if j + 1 >= slabs else 1 + (slab + j + 1 < slabs).astype(jnp.int32)
                    pl.semaphore_wait(slab_ready.at[j // 2 - 1], others)
                slab_copies[j].start()

    def interior_one(r, t):
        first_pass(r, t)
        inner_face(first, r, t)

    split = jnp.where(slab + wedge > 0, 2, rows - 2)
    begun = jnp.where(slab + wedge > 0, 1, 2)
    each_row(0, begun, all_tiles(first_pass))
    each_row(2, split, all_tiles(interior_one))
    pl.when(greeted > 0)(lambda: pl.semaphore_wait(barrier, greeted))
    for j in range(1, wedges):
        signal(phi_ready.at[0], at_peer(0, -j), wedge >= j)
    for j in range(2, slabs):
        signal(slab_ready.at[j // 2 - 1], at_peer(-j), slab >= j)

    def first_down():
        for copies in first_radial:
            down_start(copies)

    for j in range(1, wedges):
        pl.when(wedge + j >= wedges)(wedge_copies[j - 1].start)
    pl.when(is_inner)(first_down)
    for copies in first_radial:
        up_start(copies)
    pl.when(is_outer)(first_down)
    for side, jump in beside:
        pl.when(wedge + jump >= wedges)(first_phi[side].start)
    lax.fori_loop(
        begun - 1, 3,
        lambda i, _: (all_tiles(first_pass)(jnp.where(i == 0, 1, rows - 3 + i)), 0)[1], 0,
    )

    @pl.when(wedge + 1 < wedges)
    def _():
        pl.semaphore_wait(phi_ready.at[0], wedges - 1 - wedge)

    for j in range(1, wedges):
        pl.when(wedge + j < wedges)(wedge_copies[j - 1].start)
    for side, jump in beside:
        pl.when(wedge + jump < wedges)(first_phi[side].start)
    each_row(split, rows - 2, all_tiles(interior_one))
    each_row(rows - 2, rows - 1, all_tiles(lambda f, t: inner_face(first, f, t)))
    await_bytes(wedge_got.at[pl.ds(1, wedges - 1)], mass_recv.at[0])
    own = jnp.zeros((1, lanes), jnp.float32)
    for w in range(wedges):
        own = own + wedge_got[lax.rem(wedge + wedges - w, wedges)]
    slab_part[...] = own
    pl.when(has_down)(slab_back.start)
    slab_start(1, 4)
    await_bytes(halo.at[pl.ds(0, 2)], phi_recv.at[0])
    for side in range(2):
        phi_unpack(first, 0, side, whole)
    each_edge(all_tiles(phi_one))

    def radial_side(step, copies, buffer, after, then=None):
        low = half == step
        for t in range(tiles):
            pl.when(low)(lambda: low_land(copies[t], buffer, t, after))
            pl.when(jnp.logical_not(low))(lambda: high_land(copies[t], buffer, t, after))
            side_faces(buffer, low, t)
            if then:
                then(t)

    def row_of(i):
        return jnp.where(is_inner, i, rows - 1 - i)

    def each_from(low, high, step):
        each_row(low, high, lambda i: step(row_of(i)))

    def passing_start(copies, gates, which, chosen):
        for t in chosen:
            @pl.when(which)
            def _():
                pl.when(is_inner & has_up)(gates[t][0].wait_send)
                pl.when(is_outer & has_down)(gates[t][1].wait_send)
                pl.when(is_inner)(lambda: down_start(copies[t]))
                pl.when(is_outer)(lambda: up_start(copies[t]))

    def phi_leave(copies, piece):
        for side, copy in enumerate(copies):
            phi_pack(second, 1, side, piece)
            copy.start()

    def phi_land(slot, piece):
        begin, count = piece
        await_bytes(halo.at[pl.ds(2, 2), :, pl.ds(begin, count)], phi_recv.at[slot])
        for side in range(2):
            phi_unpack(second, 1, side, piece)
            each_row(2 + begin, 2 + begin + count, lambda p: gravity(p, -1 if side else tiles))

    span = (rows + 4, lanes)
    lane = lax.broadcasted_iota(jnp.int32, span, 1)
    line = lax.broadcasted_iota(jnp.int32, span, 0) - 2

    def below(row):
        return jnp.where(lane < row, 1.0, jnp.where(lane == row, 0.5, 0.0))

    def above(row):
        return jnp.where(lane > row, 1.0, jnp.where(lane == row, 0.5, 0.0))

    further = INNER_RADIUS + (
        (slab * rows + line).astype(jnp.float32) + 0.5
    ) * radial_step

    def masses():
        load_core.wait()
        for j in range(1, slabs):
            @pl.when(slab == j)
            def _():
                await_bytes(slab_got.at[pl.ds(1, j)], mass_recv.at[1])

        before = jnp.zeros((1, lanes), jnp.float32)
        for j in range(slabs - 1, 0, -1):
            before = before + slab_got[j]
        enclosed = below(line) * slab_part[...] + (before - above(line + rows) * slab_got[1])
        enclosed = core[0] + jnp.sum(enclosed, axis=1, keepdims=True) + jnp.zeros(span, jnp.float32)
        mass_ref[...] = jnp.sum(jnp.where(lane == line, enclosed, 0.0), axis=0, keepdims=True)[:, :rows]
        pull[...] = strength * enclosed / (further * further)

        each_from(0, rows - 2, all_tiles(lambda r, t: gravity(r + 2, t)))

    slab_start(4, 6)
    radial_side(0, first_radial, first, None)
    slab_start(6, slabs)
    passing_start(second_radial, first_radial, is_inner, range(tiles))
    each_row(2, rows - 2, all_tiles(phi_one))
    phi_leave(main_phi, main)
    ahead = jnp.where(is_inner, rows - 4, 0)
    pl.when(is_inner)(masses)
    each_from(0, ahead, all_tiles(theta_two))

    def second_start(t):
        pl.when(is_inner)(lambda: up_start(second_radial[t]))
        pl.when(is_outer)(lambda: down_start(second_radial[t]))
        passing_start(second_radial, first_radial, is_outer, [t])

    radial_side(
        1, first_radial, first, None,
        second_start,
    )
    phi_leave(late_phi, late)
    pl.when(is_outer)(masses)
    each_from(rows - 2, rows, all_tiles(lambda r, t: gravity(r + 2, t)))
    each_from(ahead, rows, all_tiles(theta_two))
    each_row(2, rows - 1, all_tiles(lambda f, t: inner_face(second, f, t)))
    phi_land(1, main)
    each_from(0, rows - 2, all_tiles(phi_two))
    phi_land(2, late)
    each_from(rows - 2, rows, all_tiles(phi_two))

    @pl.when(has_up)
    def _():
        slab_back.wait_recv()
        beyond = jnp.sum(below(line - rows) * slab_got[0], axis=1, keepdims=True)
        pull[...] = pull[...] + strength * beyond / (further * further)

    radial_side(0, second_radial, second, gravity)
    radial_side(1, second_radial, second, gravity)

    await_bytes(halo, phi_send.at[0])
    await_bytes(wedge_got.at[pl.ds(1, wedges - 1)], mass_send.at[0])
    for j in range(slabs):
        @pl.when(slab == j)
        def _():
            await_bytes(slab_got.at[pl.ds(0, slabs - 1 - j + min(j, 1))], mass_send.at[1])

    for up, down in first_radial:
        pl.when(has_up & is_outer)(up.wait_send)
        pl.when(has_down & is_inner)(down.wait_send)
    def second_sent(sides):
        moved = second.at[:, pl.ds(0, 2 * sides), pl.ds(PAD, cells), :]
        await_bytes(moved, radial_send.at[2 * tiles])

    pl.when(has_up & has_down)(lambda: second_sent(2))
    pl.when(has_up != has_down)(lambda: second_sent(1))


def store(advanced_ref, mass_ref, advanced_out, mass_out, sem):
    copies = [
        pltpu.make_async_copy(advanced_ref, advanced_out, sem.at[0]),
        pltpu.make_async_copy(mass_ref, mass_out, sem.at[1]),
    ]
    for copy in copies:
        copy.start()
    for copy in copies:
        copy.wait()


def body(conserved, core_mass):
    variables, rows, cells, lanes = conserved.shape
    slabs, wedges = lax.axis_size("radial"), lax.axis_size("phi")
    sizes = step_sizes(rows * slabs, cells * wedges, lanes)
    table = jnp.asarray(angle_tables(lanes, sizes[1]))
    tiles = cells // TILE
    padded = (variables, rows + 4, cells + 2 * PAD, lanes)
    vmem = pl.BlockSpec(memory_space=pltpu.VMEM)
    hbm = pl.BlockSpec(memory_space=pltpu.HBM)
    dma = pltpu.SemaphoreType.DMA
    advanced, mass = pl.pallas_call(
        functools.partial(kernel, sizes, (slabs, wedges)),
        out_shape=(
            pltpu.VMEM(conserved.shape, jnp.float32),
            pltpu.VMEM((1, rows), jnp.float32),
        ),
        in_specs=[pl.BlockSpec(memory_space=pl.ANY)] * 3,
        out_specs=(vmem, vmem),
        scratch_shapes=[
            pltpu.VMEM(padded, jnp.float32),
            pltpu.VMEM(padded, jnp.float32),
            pltpu.VMEM((4, variables, rows, 2, lanes), jnp.float32),
            pltpu.VMEM((4, variables, rows, 2, lanes), jnp.float32),
            pltpu.VMEM((1, lanes), jnp.float32),
            pltpu.VMEM((1, lanes), jnp.float32),
            pltpu.VMEM((wedges, 1, lanes), jnp.float32),
            pltpu.VMEM((slabs, 1, lanes), jnp.float32),
            pltpu.VMEM((2,) + padded[1:], jnp.float32),
            pltpu.VMEM((rows + 4, lanes), jnp.float32),
            pltpu.VMEM((TILE, lanes), jnp.float32),
            pltpu.SMEM((1,), jnp.float32),
            dma((3,)),
            dma((2 * tiles + 1,)),
            dma((4 * tiles,)),
            dma((1,)),
            dma((3,)),
            dma((2,)),
            dma((3,)),
            pltpu.SemaphoreType.REGULAR((1,)),
            pltpu.SemaphoreType.REGULAR((max(slabs // 2, 1),)),
        ],
        compiler_params=pltpu.CompilerParams(collective_id=0, has_side_effects=True),
    )(core_mass, table, conserved)
    return pl.pallas_call(
        store,
        out_shape=(
            jax.ShapeDtypeStruct(conserved.shape, jnp.float32),
            jax.ShapeDtypeStruct((rows,), jnp.float32),
        ),
        in_specs=[pl.BlockSpec(memory_space=pl.ANY)] * 2,
        out_specs=(hbm, hbm),
        scratch_shapes=[dma((2,))],
        compiler_params=pltpu.CompilerParams(vmem_limit_bytes=4 * 2**20),
    )(advanced, mass.reshape(rows))


def solution(mesh):
    in_specs = (P(None, "radial", "phi", None), P())
    out_specs = (P(None, "radial", "phi", None), P("radial"))
    return jax.shard_map(body, mesh=mesh, in_specs=in_specs, out_specs=out_specs, check_vma=False)
```

```python
import functools
import math

import jax
import jax.numpy as jnp
import numpy as np
from jax import lax
from jax.experimental import pallas as pl
from jax.experimental.pallas import tpu as pltpu
from jax.sharding import PartitionSpec as P

ADIABATIC = 4.0 / 3.0
INNER_RADIUS = 1.0
OUTER_RADIUS = 2.0
COURANT = 0.4
GRAVITY_KICK = 0.004
MINIMUM_DENSITY = 0.05
PRESSURE_FLOOR = 0.01
MESH = pl.DeviceIdType.MESH
TILE = 8
PAD = 8


def step_sizes(radial_total, phi_total, theta_total):
    theta_step = math.pi / theta_total
    phi_step = 2.0 * math.pi / phi_total
    polar_width = INNER_RADIUS * math.sin(0.5 * theta_step) * phi_step
    radial_step = min(2.0 * polar_width, (OUTER_RADIUS - INNER_RADIUS) / radial_total)
    timestep = COURANT * min(radial_step, polar_width)
    return (radial_step, theta_step, phi_step, timestep)


def angle_tables(theta_cells, theta_step):
    step = np.float32(theta_step)
    centre = (np.arange(theta_cells, dtype=np.float32) + np.float32(0.5)) * step
    face = np.arange(theta_cells + 1, dtype=np.float32) * step
    sine = np.sin(centre.astype(np.float64))
    cosine = np.cos(centre.astype(np.float64))
    face_sine = np.sin(face.astype(np.float64))
    zero = np.zeros(theta_cells)
    rows = [sine, face_sine[:-1], face_sine[1:], cosine / sine, 1.0 / sine, zero, zero, zero]
    return np.stack(rows).astype(np.float32)


def half_slope(below, above):
    return 0.5 * jnp.maximum(
        jnp.minimum(below, above), jnp.minimum(jnp.maximum(below, above), 0.0)
    )


def thermo(q):
    density = jnp.maximum(q[0], MINIMUM_DENSITY)
    inverse = 1.0 / density
    kinetic = 0.5 * (q[1] * q[1] + q[2] * q[2] + q[3] * q[3]) * inverse
    pressure = jnp.maximum((ADIABATIC - 1.0) * (q[4] - kinetic), PRESSURE_FLOOR * density)
    return density, inverse, pressure


def physical(q, component):
    _, inverse, pressure = thermo(q)
    normal = q[component] * inverse
    squared = ADIABATIC * pressure * inverse
    return normal, pressure, jnp.abs(normal) + squared * lax.rsqrt(squared)


def flux(left, right, component):
    left_v, left_p, left_a = physical(left, component)
    right_v, right_p, right_a = physical(right, component)
    signal = jnp.maximum(left_a, right_a)
    left_w = 0.5 * (left_v + signal)
    right_w = 0.5 * (right_v - signal)
    out = [a * left_w + b * right_w for a, b in zip(left, right)]
    out[component] = out[component] + 0.5 * (left_p + right_p)
    out[4] = out[4] + 0.5 * (left_p * left_v + right_p * right_v)
    return out


def two_faces(rows, component):
    lower_left, lower_right, upper_left, upper_right = [], [], [], []
    for a, b, c, d, e in zip(*rows):
        ab, bc, cd, de = b - a, c - b, d - c, e - d
        sb, sc, sd = half_slope(ab, bc), half_slope(bc, cd), half_slope(cd, de)
        lower_left.append(b + sb)
        lower_right.append(c - sc)
        upper_left.append(c + sc)
        upper_right.append(d - sd)
    return flux(lower_left, lower_right, component), flux(upper_left, upper_right, component)


def one_face(rows, component):
    left, right = [], []
    for a, b, c, d in zip(*rows):
        ab, bc, cd = b - a, c - b, d - c
        left.append(b + half_slope(ab, bc))
        right.append(c - half_slope(bc, cd))
    return flux(left, right, component)


def kernel(
    sizes,
    counts,
    core_ref,
    table_ref,
    input_ref,
    out_ref,
    mass_ref,
    first,
    second,
    edge,
    halo,
    part,
    slab_part,
    wedge_got,
    slab_got,
    heavy,
    pull,
    table,
    core,
    load_sem,
    radial_send,
    radial_recv,
    phi_send,
    phi_recv,
    mass_send,
    mass_recv,
    phi_ready,
    slab_ready,
):
    radial_step, theta_step, phi_step, timestep = sizes
    slabs, wedges = counts
    variables, rows, cells, lanes = input_ref.shape
    tiles = cells // TILE
    strength = GRAVITY_KICK / timestep
    slab, wedge = lax.axis_index("radial"), lax.axis_index("phi")
    half = lax.rem(slab, 2)
    is_outer, is_inner = half == 1, half == 0
    has_up, has_down = slab < slabs - 1, slab > 0

    load = pltpu.make_async_copy(
        input_ref, first.at[:, pl.ds(2, rows), pl.ds(PAD, cells), :], load_sem.at[0]
    )
    load_table = pltpu.make_async_copy(table_ref, table, load_sem.at[1])
    load_core = pltpu.make_async_copy(core_ref, core, load_sem.at[2])
    for copy in (load, load_table, load_core):
        copy.start()
    slab_got[...] = jnp.zeros(slab_got.shape, jnp.float32)

    def at_peer(jump, turn=0):
        around = lax.rem(wedge + turn + wedges, wedges) if turn else wedge
        return (lax.rem(slab + jump + slabs, slabs), around)

    barrier = pltpu.get_barrier_semaphore()

    def signal(sem, peer, condition):
        @pl.when(condition)
        def _():
            pl.semaphore_signal(sem, inc=1, device_id=peer, device_id_type=MESH)

    signal(barrier, at_peer(1), has_up)
    signal(barrier, at_peer(-1), has_down)
    for j in range(1, wedges):
        signal(barrier, at_peer(0, j), wedge + j < wedges)
    for j in range(2, slabs):
        signal(barrier, at_peer(j), slab + j < slabs)
    greeted = wedge + slab + jnp.where(has_up, 1, 0)
    def remote(src, dst, send, recv, peer):
        return pltpu.make_async_remote_copy(
            src_ref=src, dst_ref=dst, send_sem=send, recv_sem=recv, device_id=peer,
            device_id_type=MESH,
        )

    def await_bytes(ref, sem):
        pltpu.make_async_copy(ref, ref, sem).wait()

    def radial_copies(buffer, section, tile):
        where = pl.ds(PAD + TILE * tile, TILE)
        slot = (section * tiles + tile) * 2
        up = remote(
            buffer.at[:, pl.ds(rows, 2), where, :], buffer.at[:, pl.ds(0, 2), where, :],
            radial_send.at[slot if section == 0 else 2 * tiles], radial_recv.at[slot], at_peer(1),
        )
        down = remote(
            buffer.at[:, pl.ds(2, 2), where, :], buffer.at[:, pl.ds(rows + 2, 2), where, :],
            radial_send.at[slot + 1 if section == 0 else 2 * tiles], radial_recv.at[slot + 1],
            at_peer(-1),
        )
        return up, down

    first_radial = [radial_copies(first, 0, t) for t in range(tiles)]
    second_radial = [radial_copies(second, 1, t) for t in range(tiles)]

    def up_start(copies):
        pl.when(has_up)(copies[0].start)

    def down_start(copies):
        pl.when(has_down)(copies[1].start)

    whole = (0, rows)
    main = (jnp.where(is_inner, 0, 2), rows - 2)
    late = (jnp.where(is_inner, rows - 2, 0), 2)

    def phi_copies(section, piece, slot):
        where = pl.ds(*piece)
        return [
            remote(
                edge.at[section * 2 + side, :, where], halo.at[section * 2 + side, :, where],
                phi_send.at[0], phi_recv.at[slot], at_peer(0, jump),
            )
            for side, jump in ((0, -1), (1, 1))
        ]

    def phi_pack(buffer, section, side, piece):
        begin, count = piece
        start = PAD if side == 0 else PAD + cells - 2
        edge[section * 2 + side, :, pl.ds(begin, count)] = buffer[
            :, pl.ds(2 + begin, count), pl.ds(start, 2), :
        ]

    def phi_unpack(buffer, section, side, piece):
        begin, count = piece
        start = PAD + cells if side == 0 else PAD - 2
        buffer[:, pl.ds(2 + begin, count), pl.ds(start, 2), :] = halo[
            section * 2 + side, :, pl.ds(begin, count)
        ]

    first_phi = phi_copies(0, whole, 0)
    main_phi, late_phi = phi_copies(1, main, 1), phi_copies(1, late, 2)

    wedge_copies = [
        remote(part, wedge_got.at[j], mass_send.at[0], mass_recv.at[0], at_peer(0, j))
        for j in range(1, wedges)
    ]
    slab_copies = {
        j: remote(slab_part, slab_got.at[j], mass_send.at[1], mass_recv.at[1], at_peer(j))
        for j in range(1, slabs)
    }
    slab_back = remote(
        slab_part, slab_got.at[0], mass_send.at[1], mass_recv.at[2], at_peer(-1)
    )
    beside = ((0, wedges - 1), (1, 1))

    load.wait()
    load_table.wait()
    shape = (TILE, lanes)
    lane = lax.broadcasted_iota(jnp.int32, (rows, lanes), 1)
    line = lax.broadcasted_iota(jnp.int32, (rows, lanes), 0)
    column = jnp.sum(first[0, pl.ds(2, rows), pl.ds(PAD, cells), :], axis=1)
    column = jnp.sum(column * table[0:1, :], axis=1, keepdims=True)
    centres = INNER_RADIUS + (
        (slab * rows + line).astype(jnp.float32) + 0.5
    ) * radial_step
    column = column * centres * centres * (radial_step * theta_step * phi_step)
    part[...] = jnp.sum(jnp.where(lane == line, column, 0.0), axis=0, keepdims=True)
    wedge_got[0] = part[...]
    phi_pack(first, 0, 0, whole)
    phi_pack(first, 0, 1, whole)

    lane_tile = lax.broadcasted_iota(jnp.int32, shape, 1)
    is_first, is_last = lane_tile == 0, lane_tile == lanes - 1

    def fields_at(buffer, row, start):
        where = pl.ds(start, TILE)
        fields = [buffer.at[k] for k in range(variables)]
        if buffer is second:
            fields[1], fields[4] = heavy.at[0], heavy.at[1]
        return [field[row + 2, where, :] for field in fields]

    def radius_at(position):
        step = jnp.full(shape, slab * rows + position, jnp.int32).astype(jnp.float32)
        return INNER_RADIUS + step * radial_step

    def face_scale(face, row):
        area, inverse_r = radius_at(face), 1.0 / (radius_at(row) + 0.5 * radial_step)
        return area * area * (inverse_r * inverse_r * (1.0 / radial_step))

    def add_flux(buffer, row, tile, scale, values):
        if buffer is first:
            target, row, start, step = second, row + 2, PAD + TILE * tile, timestep
        else:
            target, start, step = out_ref, TILE * tile, 0.5 * timestep
        scale = scale * step
        where = pl.ds(start, TILE)
        for k in range(variables):
            target[k, row, where, :] = target[k, row, where, :] + scale * values[k]

    def inner_face(buffer, face, tile):
        start = PAD + TILE * tile
        values = one_face([fields_at(buffer, face + o, start) for o in range(-2, 2)], 1)
        add_flux(buffer, face - 1, tile, -face_scale(face, face - 1), values)
        add_flux(buffer, face, tile, face_scale(face, face), values)

    def side_faces(buffer, low, tile):
        start = PAD + TILE * tile
        edge_row = jnp.where(low, 0, rows - 1)
        next_row = jnp.where(low, 1, rows - 2)
        lower, upper = two_faces([fields_at(buffer, edge_row + o, start) for o in range(-2, 3)], 1)
        low_scale, high_scale = face_scale(edge_row, edge_row), face_scale(edge_row + 1, edge_row)
        values = [low_scale * a - high_scale * b for a, b in zip(lower, upper)]
        add_flux(buffer, edge_row, tile, 1.0, values)
        between = [jnp.where(low, b, a) for a, b in zip(lower, upper)]
        scale = face_scale(jnp.where(low, 1, rows - 1), next_row)
        add_flux(buffer, next_row, tile, jnp.where(low, scale, -scale), between)

    def rate(buffer, r, tile, around_phi=True, along_theta=True):
        start = PAD + TILE * tile

        def at(row, offset):
            return fields_at(buffer, row, start + offset)

        def spread(value):
            return jnp.broadcast_to(value, shape)

        index = jnp.full(shape, slab * rows + r, jnp.int32).astype(jnp.float32)
        radius = INNER_RADIUS + (index + 0.5) * radial_step
        inverse_r = 1.0 / radius
        centre = at(r, 0)
        total = [0.0] * variables
        around = inverse_r * spread(table[4:5, :])
        if around_phi:
            lower, upper = two_faces([at(r, o) if o else centre for o in range(-2, 3)], 3)
            scale = around * (1.0 / phi_step)
            total = [t + (a - b) * scale for t, a, b in zip(total, lower, upper)]
        if not along_theta:
            return centre, total
        left, right = [], []
        for q in centre:
            after = jnp.where(is_last, q, pltpu.roll(q, lanes - 1, 1))
            above = after - q
            below = jnp.where(is_first, 0.0, pltpu.roll(above, 1, 1))
            slope = half_slope(below, above)
            left.append(q + slope)
            right.append(jnp.where(is_last, q, pltpu.roll(q - slope, lanes - 1, 1)))
        upper = flux(left, right, 2)
        scale = around * (1.0 / theta_step)
        low_sine, high_sine = spread(table[1:2, :]), spread(table[2:3, :])
        low_area, high_area = low_sine * scale, high_sine * scale
        total = [
            t + (low_area * pltpu.roll(f, 1, 1) - high_area * f) for t, f in zip(total, upper)
        ]
        density, inverse, pressure = thermo(centre)
        vr, vt, vp = (centre[m] * inverse for m in (1, 2, 3))
        cot = spread(table[3:4, :])
        total[1] = total[1] + (2.0 * pressure + density * (vt * vt + vp * vp)) * inverse_r
        total[2] = total[2] + (
            (pressure + density * vp * vp) * cot - density * vr * vt
        ) * inverse_r
        total[3] = total[3] - density * vp * (vr + vt * cot) * inverse_r
        return centre, total

    def first_pass(r, tile):
        centre, total = rate(first, r, tile, around_phi=False)
        where = pl.ds(PAD + TILE * tile, TILE)
        for k in range(variables):
            second[k, r + 2, where, :] = centre[k] + timestep * total[k]

    def phi_one(r, tile):
        _, total = rate(first, r, tile, along_theta=False)
        where = pl.ds(PAD + TILE * tile, TILE)
        for k in range(variables):
            second[k, r + 2, where, :] = second[k, r + 2, where, :] + timestep * total[k]

    def gravity(p, tile):
        where = pl.ds(PAD + TILE * tile, TILE)
        kick = timestep * jnp.broadcast_to(pull[pl.ds(p, 1), :], shape)
        density = jnp.maximum(first[0, p, where, :], MINIMUM_DENSITY)
        heavy[0, p, where, :] = second[1, p, where, :] - density * kick
        heavy[1, p, where, :] = second[4, p, where, :] - first[1, p, where, :] * kick

    def theta_two(r, tile):
        centre, total = rate(second, r, tile, around_phi=False)
        force = jnp.broadcast_to(pull[pl.ds(r + 2, 1), :], shape)
        density = jnp.maximum(centre[0], MINIMUM_DENSITY)
        total[1] = total[1] - density * force
        total[4] = total[4] - centre[1] * force
        where = pl.ds(PAD + TILE * tile, TILE)
        into = pl.ds(TILE * tile, TILE)
        for k in range(variables):
            begin = first[k, r + 2, where, :]
            out_ref[k, r, into, :] = 0.5 * begin + 0.5 * (centre[k] + timestep * total[k])

    def phi_two(r, tile):
        _, total = rate(second, r, tile, along_theta=False)
        into = pl.ds(TILE * tile, TILE)
        for k in range(variables):
            out_ref[k, r, into, :] = out_ref[k, r, into, :] + (0.5 * timestep) * total[k]

    def each_row(low, high, step):
        lax.fori_loop(low, high, lambda r, _: (step(r), 0)[1], 0)

    def each_edge(step):
        lax.fori_loop(
            0, 4, lambda i, _: (step(i + (i // 2) * (rows - 4)), 0)[1], 0
        )

    def all_tiles(step):
        def run(r):
            for t in range(tiles):
                step(r, t)

        return run

    def low_land(copies, buffer, tile, after=None):
        where = pl.ds(PAD + TILE * tile, TILE)

        @pl.when(has_down)
        def _():
            copies[0].wait_recv()
            if after:
                after(0, tile)
                after(1, tile)

        @pl.when(jnp.logical_not(has_down))
        def _():
            value = buffer[:, 2, where, :]
            buffer[:, 0, where, :] = value
            buffer[:, 1, where, :] = value
            if buffer is second:
                value = heavy[:, 2, where, :]
                heavy[:, 0, where, :] = value
                heavy[:, 1, where, :] = value

    def high_land(copies, buffer, tile, after=None):
        where = pl.ds(PAD + TILE * tile, TILE)

        @pl.when(has_up)
        def _():
            copies[1].wait_recv()
            if after:
                after(rows + 2, tile)
                after(rows + 3, tile)

        @pl.when(jnp.logical_not(has_up))
        def _():
            value = buffer[:, rows + 1, where, :]
            buffer[:, rows + 2, where, :] = value
            buffer[:, rows + 3, where, :] = value
            if buffer is second:
                value = heavy[:, rows + 1, where, :]
                heavy[:, rows + 2, where, :] = value
                heavy[:, rows + 3, where, :] = value

    def slab_start(low, high):
        for j in range(low, min(high, slabs)):
            @pl.when(slab + j < slabs)
            def _():
                if j > 1 and j % 2 == 0:
                    others = 1 if j + 1 >= slabs else 1 + (slab + j + 1 < slabs).astype(jnp.int32)
                    pl.semaphore_wait(slab_ready.at[j // 2 - 1], others)
                slab_copies[j].start()

    def interior_one(r, t):
        first_pass(r, t)
        inner_face(first, r, t)

    split = jnp.where(slab + wedge > 0, 2, rows - 2)
    begun = jnp.where(slab + wedge > 0, 1, 2)
    each_row(0, begun, all_tiles(first_pass))
    each_row(2, split, all_tiles(interior_one))
    pl.when(greeted > 0)(lambda: pl.semaphore_wait(barrier, greeted))
    for j in range(1, wedges):
        signal(phi_ready.at[0], at_peer(0, -j), wedge >= j)
    for j in range(2, slabs):
        signal(slab_ready.at[j // 2 - 1], at_peer(-j), slab >= j)

    def first_down():
        for copies in first_radial:
            down_start(copies)

    for j in range(1, wedges):
        pl.when(wedge + j >= wedges)(wedge_copies[j - 1].start)
    pl.when(is_inner)(first_down)
    for copies in first_radial:
        up_start(copies)
    pl.when(is_outer)(first_down)
    for side, jump in beside:
        pl.when(wedge + jump >= wedges)(first_phi[side].start)
    lax.fori_loop(
        begun - 1, 3,
        lambda i, _: (all_tiles(first_pass)(jnp.where(i == 0, 1, rows - 3 + i)), 0)[1], 0,
    )

    @pl.when(wedge + 1 < wedges)
    def _():
        pl.semaphore_wait(phi_ready.at[0], wedges - 1 - wedge)

    for j in range(1, wedges):
        pl.when(wedge + j < wedges)(wedge_copies[j - 1].start)
    for side, jump in beside:
        pl.when(wedge + jump < wedges)(first_phi[side].start)
    each_row(split, rows - 2, all_tiles(interior_one))
    each_row(rows - 2, rows - 1, all_tiles(lambda f, t: inner_face(first, f, t)))
    await_bytes(wedge_got.at[pl.ds(1, wedges - 1)], mass_recv.at[0])
    own = jnp.zeros((1, lanes), jnp.float32)
    for w in range(wedges):
        own = own + wedge_got[lax.rem(wedge + wedges - w, wedges)]
    slab_part[...] = own
    pl.when(has_down)(slab_back.start)
    slab_start(1, 4)
    await_bytes(halo.at[pl.ds(0, 2)], phi_recv.at[0])
    for side in range(2):
        phi_unpack(first, 0, side, whole)
    each_edge(all_tiles(phi_one))

    def radial_side(step, copies, buffer, after, then=None):
        low = half == step
        for t in range(tiles):
            pl.when(low)(lambda: low_land(copies[t], buffer, t, after))
            pl.when(jnp.logical_not(low))(lambda: high_land(copies[t], buffer, t, after))
            side_faces(buffer, low, t)
            if then:
                then(t)

    def row_of(i):
        return jnp.where(is_inner, i, rows - 1 - i)

    def each_from(low, high, step):
        each_row(low, high, lambda i: step(row_of(i)))

    def passing_start(copies, gates, which, chosen):
        for t in chosen:
            @pl.when(which)
            def _():
                pl.when(is_outer & has_down)(gates[t][1].wait_send)
                pl.when(is_inner)(lambda: down_start(copies[t]))
                pl.when(is_outer)(lambda: up_start(copies[t]))

    def phi_leave(copies, piece):
        for side, copy in enumerate(copies):
            phi_pack(second, 1, side, piece)
            copy.start()

    def phi_land(slot, piece):
        begin, count = piece
        await_bytes(halo.at[pl.ds(2, 2), :, pl.ds(begin, count)], phi_recv.at[slot])
        for side in range(2):
            phi_unpack(second, 1, side, piece)
            each_row(2 + begin, 2 + begin + count, lambda p: gravity(p, -1 if side else tiles))

    span = (rows + 4, lanes)
    lane = lax.broadcasted_iota(jnp.int32, span, 1)
    line = lax.broadcasted_iota(jnp.int32, span, 0) - 2

    def below(row):
        return jnp.where(lane < row, 1.0, jnp.where(lane == row, 0.5, 0.0))

    def above(row):
        return jnp.where(lane > row, 1.0, jnp.where(lane == row, 0.5, 0.0))

    further = INNER_RADIUS + (
        (slab * rows + line).astype(jnp.float32) + 0.5
    ) * radial_step

    def masses():
        load_core.wait()
        for j in range(1, slabs):
            @pl.when(slab == j)
            def _():
                await_bytes(slab_got.at[pl.ds(1, j)], mass_recv.at[1])

        before = jnp.zeros((1, lanes), jnp.float32)
        for j in range(slabs - 1, 0, -1):
            before = before + slab_got[j]
        enclosed = below(line) * slab_part[...] + (before - above(line + rows) * slab_got[1])
        enclosed = core[0] + jnp.sum(enclosed, axis=1, keepdims=True) + jnp.zeros(span, jnp.float32)
        mass_ref[...] = jnp.sum(jnp.where(lane == line, enclosed, 0.0), axis=0, keepdims=True)[:, :rows]
        pull[...] = strength * enclosed / (further * further)

        each_from(0, rows - 2, all_tiles(lambda r, t: gravity(r + 2, t)))

    slab_start(4, 6)
    radial_side(0, first_radial, first, None)
    slab_start(6, slabs)
    passing_start(second_radial, first_radial, is_inner, range(tiles))
    each_row(2, rows - 2, all_tiles(phi_one))
    phi_leave(main_phi, main)
    ahead = jnp.where(is_inner, rows - 3, 0)
    pl.when(is_inner)(masses)
    each_from(0, ahead, all_tiles(theta_two))

    def second_start(t):
        pl.when(is_inner)(lambda: up_start(second_radial[t]))
        pl.when(is_outer)(lambda: down_start(second_radial[t]))
        passing_start(second_radial, first_radial, is_outer, [t])

    radial_side(
        1, first_radial, first, None,
        second_start,
    )
    phi_leave(late_phi, late)
    pl.when(is_outer)(masses)
    each_from(rows - 2, rows, all_tiles(lambda r, t: gravity(r + 2, t)))
    each_from(ahead, rows, all_tiles(theta_two))
    each_row(2, rows - 1, all_tiles(lambda f, t: inner_face(second, f, t)))
    phi_land(1, main)
    each_from(0, rows - 2, all_tiles(phi_two))
    phi_land(2, late)
    each_from(rows - 2, rows, all_tiles(phi_two))

    @pl.when(has_up)
    def _():
        slab_back.wait_recv()
        beyond = jnp.sum(below(line - rows) * slab_got[0], axis=1, keepdims=True)
        pull[...] = pull[...] + strength * beyond / (further * further)

    radial_side(0, second_radial, second, gravity)
    radial_side(1, second_radial, second, gravity)

    await_bytes(halo, phi_send.at[0])
    await_bytes(wedge_got.at[pl.ds(1, wedges - 1)], mass_send.at[0])
    for j in range(slabs):
        @pl.when(slab == j)
        def _():
            await_bytes(slab_got.at[pl.ds(0, slabs - 1 - j + min(j, 1))], mass_send.at[1])

    for up, down in first_radial:
        pl.when(has_up)(up.wait_send)
        pl.when(has_down & is_inner)(down.wait_send)
    def second_sent(sides):
        moved = second.at[:, pl.ds(0, 2 * sides), pl.ds(PAD, cells), :]
        await_bytes(moved, radial_send.at[2 * tiles])

    pl.when(has_up & has_down)(lambda: second_sent(2))
    pl.when(has_up != has_down)(lambda: second_sent(1))


def store(advanced_ref, mass_ref, advanced_out, mass_out, sem):
    copies = [
        pltpu.make_async_copy(advanced_ref, advanced_out, sem.at[0]),
        pltpu.make_async_copy(mass_ref, mass_out, sem.at[1]),
    ]
    for copy in copies:
        copy.start()
    for copy in copies:
        copy.wait()


def body(conserved, core_mass):
    variables, rows, cells, lanes = conserved.shape
    slabs, wedges = lax.axis_size("radial"), lax.axis_size("phi")
    sizes = step_sizes(rows * slabs, cells * wedges, lanes)
    table = jnp.asarray(angle_tables(lanes, sizes[1]))
    tiles = cells // TILE
    padded = (variables, rows + 4, cells + 2 * PAD, lanes)
    vmem = pl.BlockSpec(memory_space=pltpu.VMEM)
    hbm = pl.BlockSpec(memory_space=pltpu.HBM)
    dma = pltpu.SemaphoreType.DMA
    advanced, mass = pl.pallas_call(
        functools.partial(kernel, sizes, (slabs, wedges)),
        out_shape=(
            pltpu.VMEM(conserved.shape, jnp.float32),
            pltpu.VMEM((1, rows), jnp.float32),
        ),
        in_specs=[pl.BlockSpec(memory_space=pl.ANY)] * 3,
        out_specs=(vmem, vmem),
        scratch_shapes=[
            pltpu.VMEM(padded, jnp.float32),
            pltpu.VMEM(padded, jnp.float32),
            pltpu.VMEM((4, variables, rows, 2, lanes), jnp.float32),
            pltpu.VMEM((4, variables, rows, 2, lanes), jnp.float32),
            pltpu.VMEM((1, lanes), jnp.float32),
            pltpu.VMEM((1, lanes), jnp.float32),
            pltpu.VMEM((wedges, 1, lanes), jnp.float32),
            pltpu.VMEM((slabs, 1, lanes), jnp.float32),
            pltpu.VMEM((2,) + padded[1:], jnp.float32),
            pltpu.VMEM((rows + 4, lanes), jnp.float32),
            pltpu.VMEM((TILE, lanes), jnp.float32),
            pltpu.SMEM((1,), jnp.float32),
            dma((3,)),
            dma((2 * tiles + 1,)),
            dma((4 * tiles,)),
            dma((1,)),
            dma((3,)),
            dma((2,)),
            dma((3,)),
            pltpu.SemaphoreType.REGULAR((1,)),
            pltpu.SemaphoreType.REGULAR((max(slabs // 2, 1),)),
        ],
        compiler_params=pltpu.CompilerParams(collective_id=0, has_side_effects=True),
    )(core_mass, table, conserved)
    return pl.pallas_call(
        store,
        out_shape=(
            jax.ShapeDtypeStruct(conserved.shape, jnp.float32),
            jax.ShapeDtypeStruct((rows,), jnp.float32),
        ),
        in_specs=[pl.BlockSpec(memory_space=pl.ANY)] * 2,
        out_specs=(hbm, hbm),
        scratch_shapes=[dma((2,))],
        compiler_params=pltpu.CompilerParams(vmem_limit_bytes=4 * 2**20),
    )(advanced, mass.reshape(rows))


def solution(mesh):
    in_specs = (P(None, "radial", "phi", None), P())
    out_specs = (P(None, "radial", "phi", None), P("radial"))
    return jax.shard_map(body, mesh=mesh, in_specs=in_specs, out_specs=out_specs, check_vma=False)
```

```python
import functools
import math

import jax
import jax.numpy as jnp
import numpy as np
from jax import lax
from jax.experimental import pallas as pl
from jax.experimental.pallas import tpu as pltpu
from jax.sharding import PartitionSpec as P

ADIABATIC = 4.0 / 3.0
INNER_RADIUS = 1.0
OUTER_RADIUS = 2.0
COURANT = 0.4
GRAVITY_KICK = 0.004
MINIMUM_DENSITY = 0.05
PRESSURE_FLOOR = 0.01
MESH = pl.DeviceIdType.MESH
TILE = 8
PAD = 8


def step_sizes(radial_total, phi_total, theta_total):
    theta_step = math.pi / theta_total
    phi_step = 2.0 * math.pi / phi_total
    polar_width = INNER_RADIUS * math.sin(0.5 * theta_step) * phi_step
    radial_step = min(2.0 * polar_width, (OUTER_RADIUS - INNER_RADIUS) / radial_total)
    timestep = COURANT * min(radial_step, polar_width)
    return (radial_step, theta_step, phi_step, timestep)


def angle_tables(theta_cells, theta_step):
    step = np.float32(theta_step)
    centre = (np.arange(theta_cells, dtype=np.float32) + np.float32(0.5)) * step
    face = np.arange(theta_cells + 1, dtype=np.float32) * step
    sine = np.sin(centre.astype(np.float64))
    cosine = np.cos(centre.astype(np.float64))
    face_sine = np.sin(face.astype(np.float64))
    zero = np.zeros(theta_cells)
    rows = [sine, face_sine[:-1], face_sine[1:], cosine / sine, 1.0 / sine, zero, zero, zero]
    return np.stack(rows).astype(np.float32)


def half_slope(below, above):
    return 0.5 * jnp.maximum(
        jnp.minimum(below, above), jnp.minimum(jnp.maximum(below, above), 0.0)
    )


def thermo(q):
    density = jnp.maximum(q[0], MINIMUM_DENSITY)
    inverse = 1.0 / density
    kinetic = 0.5 * (q[1] * q[1] + q[2] * q[2] + q[3] * q[3]) * inverse
    pressure = jnp.maximum((ADIABATIC - 1.0) * (q[4] - kinetic), PRESSURE_FLOOR * density)
    return density, inverse, pressure


def physical(q, component):
    _, inverse, pressure = thermo(q)
    normal = q[component] * inverse
    squared = ADIABATIC * pressure * inverse
    return normal, pressure, jnp.abs(normal) + squared * lax.rsqrt(squared)


def flux(left, right, component):
    left_v, left_p, left_a = physical(left, component)
    right_v, right_p, right_a = physical(right, component)
    signal = jnp.maximum(left_a, right_a)
    left_w = 0.5 * (left_v + signal)
    right_w = 0.5 * (right_v - signal)
    out = [a * left_w + b * right_w for a, b in zip(left, right)]
    out[component] = out[component] + 0.5 * (left_p + right_p)
    out[4] = out[4] + 0.5 * (left_p * left_v + right_p * right_v)
    return out


def two_faces(rows, component):
    lower_left, lower_right, upper_left, upper_right = [], [], [], []
    for a, b, c, d, e in zip(*rows):
        ab, bc, cd, de = b - a, c - b, d - c, e - d
        sb, sc, sd = half_slope(ab, bc), half_slope(bc, cd), half_slope(cd, de)
        lower_left.append(b + sb)
        lower_right.append(c - sc)
        upper_left.append(c + sc)
        upper_right.append(d - sd)
    return flux(lower_left, lower_right, component), flux(upper_left, upper_right, component)


def one_face(rows, component):
    left, right = [], []
    for a, b, c, d in zip(*rows):
        ab, bc, cd = b - a, c - b, d - c
        left.append(b + half_slope(ab, bc))
        right.append(c - half_slope(bc, cd))
    return flux(left, right, component)


def kernel(
    sizes,
    counts,
    core_ref,
    table_ref,
    input_ref,
    out_ref,
    mass_ref,
    first,
    second,
    edge,
    halo,
    part,
    slab_part,
    wedge_got,
    slab_got,
    heavy,
    pull,
    table,
    core,
    load_sem,
    radial_send,
    radial_recv,
    phi_send,
    phi_recv,
    mass_send,
    mass_recv,
    phi_ready,
    slab_ready,
):
    radial_step, theta_step, phi_step, timestep = sizes
    slabs, wedges = counts
    variables, rows, cells, lanes = input_ref.shape
    tiles = cells // TILE
    strength = GRAVITY_KICK / timestep
    slab, wedge = lax.axis_index("radial"), lax.axis_index("phi")
    half = lax.rem(slab, 2)
    is_outer, is_inner = half == 1, half == 0
    has_up, has_down = slab < slabs - 1, slab > 0

    load = pltpu.make_async_copy(
        input_ref, first.at[:, pl.ds(2, rows), pl.ds(PAD, cells), :], load_sem.at[0]
    )
    load_table = pltpu.make_async_copy(table_ref, table, load_sem.at[1])
    load_core = pltpu.make_async_copy(core_ref, core, load_sem.at[2])
    for copy in (load, load_table, load_core):
        copy.start()
    slab_got[...] = jnp.zeros(slab_got.shape, jnp.float32)

    def at_peer(jump, turn=0):
        around = lax.rem(wedge + turn + wedges, wedges) if turn else wedge
        return (lax.rem(slab + jump + slabs, slabs), around)

    barrier = pltpu.get_barrier_semaphore()

    def signal(sem, peer, condition):
        @pl.when(condition)
        def _():
            pl.semaphore_signal(sem, inc=1, device_id=peer, device_id_type=MESH)

    signal(barrier, at_peer(1), has_up)
    signal(barrier, at_peer(-1), has_down)
    for j in range(1, wedges):
        signal(barrier, at_peer(0, j), wedge + j < wedges)
    for j in range(2, slabs):
        signal(barrier, at_peer(j), slab + j < slabs)
    greeted = wedge + slab + jnp.where(has_up, 1, 0)
    def remote(src, dst, send, recv, peer):
        return pltpu.make_async_remote_copy(
            src_ref=src, dst_ref=dst, send_sem=send, recv_sem=recv, device_id=peer,
            device_id_type=MESH,
        )

    def await_bytes(ref, sem):
        pltpu.make_async_copy(ref, ref, sem).wait()

    def radial_copies(buffer, section, tile):
        where = pl.ds(PAD + TILE * tile, TILE)
        slot = (section * tiles + tile) * 2
        up = remote(
            buffer.at[:, pl.ds(rows, 2), where, :], buffer.at[:, pl.ds(0, 2), where, :],
            radial_send.at[slot if section == 0 else 2 * tiles], radial_recv.at[slot], at_peer(1),
        )
        down = remote(
            buffer.at[:, pl.ds(2, 2), where, :], buffer.at[:, pl.ds(rows + 2, 2), where, :],
            radial_send.at[slot + 1 if section == 0 else 2 * tiles], radial_recv.at[slot + 1],
            at_peer(-1),
        )
        return up, down

    first_radial = [radial_copies(first, 0, t) for t in range(tiles)]
    second_radial = [radial_copies(second, 1, t) for t in range(tiles)]

    def up_start(copies):
        pl.when(has_up)(copies[0].start)

    def down_start(copies):
        pl.when(has_down)(copies[1].start)

    whole = (0, rows)
    main = (jnp.where(is_inner, 0, 2), rows - 2)
    late = (jnp.where(is_inner, rows - 2, 0), 2)

    def phi_copies(section, piece, slot):
        where = pl.ds(*piece)
        return [
            remote(
                edge.at[section * 2 + side, :, where], halo.at[section * 2 + side, :, where],
                phi_send.at[0], phi_recv.at[slot], at_peer(0, jump),
            )
            for side, jump in ((0, -1), (1, 1))
        ]

    def phi_pack(buffer, section, side, piece):
        begin, count = piece
        start = PAD if side == 0 else PAD + cells - 2
        edge[section * 2 + side, :, pl.ds(begin, count)] = buffer[
            :, pl.ds(2 + begin, count), pl.ds(start, 2), :
        ]

    def phi_unpack(buffer, section, side, piece):
        begin, count = piece
        start = PAD + cells if side == 0 else PAD - 2
        buffer[:, pl.ds(2 + begin, count), pl.ds(start, 2), :] = halo[
            section * 2 + side, :, pl.ds(begin, count)
        ]

    first_phi = phi_copies(0, whole, 0)
    main_phi, late_phi = phi_copies(1, main, 1), phi_copies(1, late, 2)

    wedge_copies = [
        remote(part, wedge_got.at[j], mass_send.at[0], mass_recv.at[0], at_peer(0, j))
        for j in range(1, wedges)
    ]
    slab_copies = {
        j: remote(slab_part, slab_got.at[j], mass_send.at[1], mass_recv.at[1], at_peer(j))
        for j in range(1, slabs)
    }
    slab_back = remote(
        slab_part, slab_got.at[0], mass_send.at[1], mass_recv.at[2], at_peer(-1)
    )
    beside = ((0, wedges - 1), (1, 1))

    load.wait()
    load_table.wait()
    shape = (TILE, lanes)
    lane = lax.broadcasted_iota(jnp.int32, (rows, lanes), 1)
    line = lax.broadcasted_iota(jnp.int32, (rows, lanes), 0)
    column = jnp.sum(first[0, pl.ds(2, rows), pl.ds(PAD, cells), :], axis=1)
    column = jnp.sum(column * table[0:1, :], axis=1, keepdims=True)
    centres = INNER_RADIUS + (
        (slab * rows + line).astype(jnp.float32) + 0.5
    ) * radial_step
    column = column * centres * centres * (radial_step * theta_step * phi_step)
    part[...] = jnp.sum(jnp.where(lane == line, column, 0.0), axis=0, keepdims=True)
    wedge_got[0] = part[...]
    phi_pack(first, 0, 0, whole)
    phi_pack(first, 0, 1, whole)

    lane_tile = lax.broadcasted_iota(jnp.int32, shape, 1)
    is_first, is_last = lane_tile == 0, lane_tile == lanes - 1

    def fields_at(buffer, row, start):
        where = pl.ds(start, TILE)
        fields = [buffer.at[k] for k in range(variables)]
        if buffer is second:
            fields[1], fields[4] = heavy.at[0], heavy.at[1]
        return [field[row + 2, where, :] for field in fields]

    def radius_at(position):
        step = jnp.full(shape, slab * rows + position, jnp.int32).astype(jnp.float32)
        return INNER_RADIUS + step * radial_step

    def face_scale(face, row):
        area, inverse_r = radius_at(face), 1.0 / (radius_at(row) + 0.5 * radial_step)
        return area * area * (inverse_r * inverse_r * (1.0 / radial_step))

    def add_flux(buffer, row, tile, scale, values):
        if buffer is first:
            target, row, start, step = second, row + 2, PAD + TILE * tile, timestep
        else:
            target, start, step = out_ref, TILE * tile, 0.5 * timestep
        scale = scale * step
        where = pl.ds(start, TILE)
        for k in range(variables):
            target[k, row, where, :] = target[k, row, where, :] + scale * values[k]

    def inner_face(buffer, face, tile):
        start = PAD + TILE * tile
        values = one_face([fields_at(buffer, face + o, start) for o in range(-2, 2)], 1)
        add_flux(buffer, face - 1, tile, -face_scale(face, face - 1), values)
        add_flux(buffer, face, tile, face_scale(face, face), values)

    def side_faces(buffer, low, tile):
        start = PAD + TILE * tile
        edge_row = jnp.where(low, 0, rows - 1)
        next_row = jnp.where(low, 1, rows - 2)
        lower, upper = two_faces([fields_at(buffer, edge_row + o, start) for o in range(-2, 3)], 1)
        low_scale, high_scale = face_scale(edge_row, edge_row), face_scale(edge_row + 1, edge_row)
        values = [low_scale * a - high_scale * b for a, b in zip(lower, upper)]
        add_flux(buffer, edge_row, tile, 1.0, values)
        between = [jnp.where(low, b, a) for a, b in zip(lower, upper)]
        scale = face_scale(jnp.where(low, 1, rows - 1), next_row)
        add_flux(buffer, next_row, tile, jnp.where(low, scale, -scale), between)

    def rate(buffer, r, tile, around_phi=True, along_theta=True):
        start = PAD + TILE * tile

        def at(row, offset):
            return fields_at(buffer, row, start + offset)

        def spread(value):
            return jnp.broadcast_to(value, shape)

        index = jnp.full(shape, slab * rows + r, jnp.int32).astype(jnp.float32)
        radius = INNER_RADIUS + (index + 0.5) * radial_step
        inverse_r = 1.0 / radius
        centre = at(r, 0)
        total = [0.0] * variables
        around = inverse_r * spread(table[4:5, :])
        if around_phi:
            lower, upper = two_faces([at(r, o) if o else centre for o in range(-2, 3)], 3)
            scale = around * (1.0 / phi_step)
            total = [t + (a - b) * scale for t, a, b in zip(total, lower, upper)]
        if not along_theta:
            return centre, total
        left, right = [], []
        for q in centre:
            after = jnp.where(is_last, q, pltpu.roll(q, lanes - 1, 1))
            above = after - q
            below = jnp.where(is_first, 0.0, pltpu.roll(above, 1, 1))
            slope = half_slope(below, above)
            left.append(q + slope)
            right.append(jnp.where(is_last, q, pltpu.roll(q - slope, lanes - 1, 1)))
        upper = flux(left, right, 2)
        scale = around * (1.0 / theta_step)
        low_sine, high_sine = spread(table[1:2, :]), spread(table[2:3, :])
        low_area, high_area = low_sine * scale, high_sine * scale
        total = [
            t + (low_area * pltpu.roll(f, 1, 1) - high_area * f) for t, f in zip(total, upper)
        ]
        density, inverse, pressure = thermo(centre)
        vr, vt, vp = (centre[m] * inverse for m in (1, 2, 3))
        cot = spread(table[3:4, :])
        total[1] = total[1] + (2.0 * pressure + density * (vt * vt + vp * vp)) * inverse_r
        total[2] = total[2] + (
            (pressure + density * vp * vp) * cot - density * vr * vt
        ) * inverse_r
        total[3] = total[3] - density * vp * (vr + vt * cot) * inverse_r
        return centre, total

    def first_pass(r, tile):
        centre, total = rate(first, r, tile, around_phi=False)
        where = pl.ds(PAD + TILE * tile, TILE)
        for k in range(variables):
            second[k, r + 2, where, :] = centre[k] + timestep * total[k]

    def phi_one(r, tile):
        _, total = rate(first, r, tile, along_theta=False)
        where = pl.ds(PAD + TILE * tile, TILE)
        for k in range(variables):
            second[k, r + 2, where, :] = second[k, r + 2, where, :] + timestep * total[k]

    def gravity(p, tile):
        where = pl.ds(PAD + TILE * tile, TILE)
        kick = timestep * jnp.broadcast_to(pull[pl.ds(p, 1), :], shape)
        density = jnp.maximum(first[0, p, where, :], MINIMUM_DENSITY)
        heavy[0, p, where, :] = second[1, p, where, :] - density * kick
        heavy[1, p, where, :] = second[4, p, where, :] - first[1, p, where, :] * kick

    def theta_two(r, tile):
        centre, total = rate(second, r, tile, around_phi=False)
        force = jnp.broadcast_to(pull[pl.ds(r + 2, 1), :], shape)
        density = jnp.maximum(centre[0], MINIMUM_DENSITY)
        total[1] = total[1] - density * force
        total[4] = total[4] - centre[1] * force
        where = pl.ds(PAD + TILE * tile, TILE)
        into = pl.ds(TILE * tile, TILE)
        for k in range(variables):
            begin = first[k, r + 2, where, :]
            out_ref[k, r, into, :] = 0.5 * begin + 0.5 * (centre[k] + timestep * total[k])

    def phi_two(r, tile):
        _, total = rate(second, r, tile, along_theta=False)
        into = pl.ds(TILE * tile, TILE)
        for k in range(variables):
            out_ref[k, r, into, :] = out_ref[k, r, into, :] + (0.5 * timestep) * total[k]

    def each_row(low, high, step):
        lax.fori_loop(low, high, lambda r, _: (step(r), 0)[1], 0)

    def each_edge(step):
        lax.fori_loop(
            0, 4, lambda i, _: (step(i + (i // 2) * (rows - 4)), 0)[1], 0
        )

    def all_tiles(step):
        def run(r):
            for t in range(tiles):
                step(r, t)

        return run

    def low_land(copies, buffer, tile, after=None):
        where = pl.ds(PAD + TILE * tile, TILE)

        @pl.when(has_down)
        def _():
            copies[0].wait_recv()
            if after:
                after(0, tile)
                after(1, tile)

        @pl.when(jnp.logical_not(has_down))
        def _():
            value = buffer[:, 2, where, :]
            buffer[:, 0, where, :] = value
            buffer[:, 1, where, :] = value
            if buffer is second:
                value = heavy[:, 2, where, :]
                heavy[:, 0, where, :] = value
                heavy[:, 1, where, :] = value

    def high_land(copies, buffer, tile, after=None):
        where = pl.ds(PAD + TILE * tile, TILE)

        @pl.when(has_up)
        def _():
            copies[1].wait_recv()
            if after:
                after(rows + 2, tile)
                after(rows + 3, tile)

        @pl.when(jnp.logical_not(has_up))
        def _():
            value = buffer[:, rows + 1, where, :]
            buffer[:, rows + 2, where, :] = value
            buffer[:, rows + 3, where, :] = value
            if buffer is second:
                value = heavy[:, rows + 1, where, :]
                heavy[:, rows + 2, where, :] = value
                heavy[:, rows + 3, where, :] = value

    def slab_start(low, high):
        for j in range(low, min(high, slabs)):
            @pl.when(slab + j < slabs)
            def _():
                if j > 1 and j % 2 == 0:
                    others = 1 if j + 1 >= slabs else 1 + (slab + j + 1 < slabs).astype(jnp.int32)
                    pl.semaphore_wait(slab_ready.at[j // 2 - 1], others)
                slab_copies[j].start()

    def interior_one(r, t):
        first_pass(r, t)
        inner_face(first, r, t)

    split = jnp.where(slab + wedge > 0, 2, rows - 2)
    begun = jnp.where(slab + wedge > 0, 1, 2)
    each_row(0, begun, all_tiles(first_pass))
    each_row(2, split, all_tiles(interior_one))
    pl.when(greeted > 0)(lambda: pl.semaphore_wait(barrier, greeted))
    for j in range(1, wedges):
        signal(phi_ready.at[0], at_peer(0, -j), wedge >= j)
    for j in range(2, slabs):
        signal(slab_ready.at[j // 2 - 1], at_peer(-j), slab >= j)

    def first_down():
        for copies in first_radial:
            down_start(copies)

    for j in range(1, wedges):
        pl.when(wedge + j >= wedges)(wedge_copies[j - 1].start)
    pl.when(is_inner)(first_down)
    for copies in first_radial:
        up_start(copies)
    pl.when(is_outer)(first_down)
    for side, jump in beside:
        pl.when(wedge + jump >= wedges)(first_phi[side].start)
    lax.fori_loop(
        begun - 1, 2,
        lambda i, _: (all_tiles(first_pass)(jnp.where(i == 0, 1, rows - 3 + i)), 0)[1], 0,
    )

    @pl.when(wedge + 1 < wedges)
    def _():
        pl.semaphore_wait(phi_ready.at[0], wedges - 1 - wedge)

    for j in range(1, wedges):
        pl.when(wedge + j < wedges)(wedge_copies[j - 1].start)
    for side, jump in beside:
        pl.when(wedge + jump < wedges)(first_phi[side].start)
    each_row(rows - 1, rows, all_tiles(first_pass))
    each_row(split, rows - 2, all_tiles(interior_one))
    each_row(rows - 2, rows - 1, all_tiles(lambda f, t: inner_face(first, f, t)))
    await_bytes(wedge_got.at[pl.ds(1, wedges - 1)], mass_recv.at[0])
    own = jnp.zeros((1, lanes), jnp.float32)
    for w in range(wedges):
        own = own + wedge_got[lax.rem(wedge + wedges - w, wedges)]
    slab_part[...] = own
    pl.when(has_down)(slab_back.start)
    slab_start(1, 4)
    await_bytes(halo.at[pl.ds(0, 2)], phi_recv.at[0])
    for side in range(2):
        phi_unpack(first, 0, side, whole)
    each_edge(all_tiles(phi_one))

    def radial_side(step, copies, buffer, after, then=None):
        low = half == step
        for t in range(tiles):
            pl.when(low)(lambda: low_land(copies[t], buffer, t, after))
            pl.when(jnp.logical_not(low))(lambda: high_land(copies[t], buffer, t, after))
            side_faces(buffer, low, t)
            if then:
                then(t)

    def row_of(i):
        return jnp.where(is_inner, i, rows - 1 - i)

    def each_from(low, high, step):
        each_row(low, high, lambda i: step(row_of(i)))

    def passing_start(copies, gates, which, chosen):
        for t in chosen:
            @pl.when(which)
            def _():
                pl.when(is_outer & has_down)(gates[t][1].wait_send)
                pl.when(is_inner)(lambda: down_start(copies[t]))
                pl.when(is_outer)(lambda: up_start(copies[t]))

    def phi_leave(copies, piece):
        for side, copy in enumerate(copies):
            phi_pack(second, 1, side, piece)
            copy.start()

    def phi_land(slot, piece):
        begin, count = piece
        await_bytes(halo.at[pl.ds(2, 2), :, pl.ds(begin, count)], phi_recv.at[slot])
        for side in range(2):
            phi_unpack(second, 1, side, piece)
            each_row(2 + begin, 2 + begin + count, lambda p: gravity(p, -1 if side else tiles))

    span = (rows + 4, lanes)
    lane = lax.broadcasted_iota(jnp.int32, span, 1)
    line = lax.broadcasted_iota(jnp.int32, span, 0) - 2

    def below(row):
        return jnp.where(lane < row, 1.0, jnp.where(lane == row, 0.5, 0.0))

    def above(row):
        return jnp.where(lane > row, 1.0, jnp.where(lane == row, 0.5, 0.0))

    further = INNER_RADIUS + (
        (slab * rows + line).astype(jnp.float32) + 0.5
    ) * radial_step

    def masses():
        load_core.wait()
        for j in range(1, slabs):
            @pl.when(slab == j)
            def _():
                await_bytes(slab_got.at[pl.ds(1, j)], mass_recv.at[1])

        before = jnp.zeros((1, lanes), jnp.float32)
        for j in range(slabs - 1, 0, -1):
            before = before + slab_got[j]
        enclosed = below(line) * slab_part[...] + (before - above(line + rows) * slab_got[1])
        enclosed = core[0] + jnp.sum(enclosed, axis=1, keepdims=True) + jnp.zeros(span, jnp.float32)
        mass_ref[...] = jnp.sum(jnp.where(lane == line, enclosed, 0.0), axis=0, keepdims=True)[:, :rows]
        pull[...] = strength * enclosed / (further * further)

        each_from(0, rows - 2, all_tiles(lambda r, t: gravity(r + 2, t)))

    slab_start(4, 6)
    radial_side(0, first_radial, first, None)
    slab_start(6, slabs)
    passing_start(second_radial, first_radial, is_inner, range(tiles))
    each_row(2, rows - 2, all_tiles(phi_one))
    phi_leave(main_phi, main)
    ahead = jnp.where(is_inner, rows - 3, 0)
    pl.when(is_inner)(masses)
    each_from(0, ahead, all_tiles(theta_two))

    def second_start(t):
        pl.when(is_inner)(lambda: up_start(second_radial[t]))
        pl.when(is_outer)(lambda: down_start(second_radial[t]))
        passing_start(second_radial, first_radial, is_outer, [t])

    radial_side(
        1, first_radial, first, None,
        second_start,
    )
    phi_leave(late_phi, late)
    pl.when(is_outer)(masses)
    each_from(rows - 2, rows, all_tiles(lambda r, t: gravity(r + 2, t)))
    each_from(ahead, rows, all_tiles(theta_two))
    each_row(2, rows - 1, all_tiles(lambda f, t: inner_face(second, f, t)))
    phi_land(1, main)
    each_from(0, rows - 2, all_tiles(phi_two))
    phi_land(2, late)
    each_from(rows - 2, rows, all_tiles(phi_two))

    @pl.when(has_up)
    def _():
        slab_back.wait_recv()
        beyond = jnp.sum(below(line - rows) * slab_got[0], axis=1, keepdims=True)
        pull[...] = pull[...] + strength * beyond / (further * further)

    radial_side(0, second_radial, second, gravity)
    radial_side(1, second_radial, second, gravity)

    await_bytes(halo, phi_send.at[0])
    await_bytes(wedge_got.at[pl.ds(1, wedges - 1)], mass_send.at[0])
    for j in range(slabs):
        @pl.when(slab == j)
        def _():
            await_bytes(slab_got.at[pl.ds(0, slabs - 1 - j + min(j, 1))], mass_send.at[1])

    for up, down in first_radial:
        pl.when(has_up)(up.wait_send)
        pl.when(has_down & is_inner)(down.wait_send)
    def second_sent(sides):
        moved = second.at[:, pl.ds(0, 2 * sides), pl.ds(PAD, cells), :]
        await_bytes(moved, radial_send.at[2 * tiles])

    pl.when(has_up & has_down)(lambda: second_sent(2))
    pl.when(has_up != has_down)(lambda: second_sent(1))


def store(advanced_ref, mass_ref, advanced_out, mass_out, sem):
    copies = [
        pltpu.make_async_copy(advanced_ref, advanced_out, sem.at[0]),
        pltpu.make_async_copy(mass_ref, mass_out, sem.at[1]),
    ]
    for copy in copies:
        copy.start()
    for copy in copies:
        copy.wait()


def body(conserved, core_mass):
    variables, rows, cells, lanes = conserved.shape
    slabs, wedges = lax.axis_size("radial"), lax.axis_size("phi")
    sizes = step_sizes(rows * slabs, cells * wedges, lanes)
    table = jnp.asarray(angle_tables(lanes, sizes[1]))
    tiles = cells // TILE
    padded = (variables, rows + 4, cells + 2 * PAD, lanes)
    vmem = pl.BlockSpec(memory_space=pltpu.VMEM)
    hbm = pl.BlockSpec(memory_space=pltpu.HBM)
    dma = pltpu.SemaphoreType.DMA
    advanced, mass = pl.pallas_call(
        functools.partial(kernel, sizes, (slabs, wedges)),
        out_shape=(
            pltpu.VMEM(conserved.shape, jnp.float32),
            pltpu.VMEM((1, rows), jnp.float32),
        ),
        in_specs=[pl.BlockSpec(memory_space=pl.ANY)] * 3,
        out_specs=(vmem, vmem),
        scratch_shapes=[
            pltpu.VMEM(padded, jnp.float32),
            pltpu.VMEM(padded, jnp.float32),
            pltpu.VMEM((4, variables, rows, 2, lanes), jnp.float32),
            pltpu.VMEM((4, variables, rows, 2, lanes), jnp.float32),
            pltpu.VMEM((1, lanes), jnp.float32),
            pltpu.VMEM((1, lanes), jnp.float32),
            pltpu.VMEM((wedges, 1, lanes), jnp.float32),
            pltpu.VMEM((slabs, 1, lanes), jnp.float32),
            pltpu.VMEM((2,) + padded[1:], jnp.float32),
            pltpu.VMEM((rows + 4, lanes), jnp.float32),
            pltpu.VMEM((TILE, lanes), jnp.float32),
            pltpu.SMEM((1,), jnp.float32),
            dma((3,)),
            dma((2 * tiles + 1,)),
            dma((4 * tiles,)),
            dma((1,)),
            dma((3,)),
            dma((2,)),
            dma((3,)),
            pltpu.SemaphoreType.REGULAR((1,)),
            pltpu.SemaphoreType.REGULAR((max(slabs // 2, 1),)),
        ],
        compiler_params=pltpu.CompilerParams(collective_id=0, has_side_effects=True),
    )(core_mass, table, conserved)
    return pl.pallas_call(
        store,
        out_shape=(
            jax.ShapeDtypeStruct(conserved.shape, jnp.float32),
            jax.ShapeDtypeStruct((rows,), jnp.float32),
        ),
        in_specs=[pl.BlockSpec(memory_space=pl.ANY)] * 2,
        out_specs=(hbm, hbm),
        scratch_shapes=[dma((2,))],
        compiler_params=pltpu.CompilerParams(vmem_limit_bytes=4 * 2**20),
    )(advanced, mass.reshape(rows))


def solution(mesh):
    in_specs = (P(None, "radial", "phi", None), P())
    out_specs = (P(None, "radial", "phi", None), P("radial"))
    return jax.shard_map(body, mesh=mesh, in_specs=in_specs, out_specs=out_specs, check_vma=False)
```
